32 devices in a mesh: head: 2 (over core), blk: 4 (over z), rep: 4 (over y, x).
Axes of the slice: x: 2, y: 2, z: 4, core: 2. Of those that a mesh axis runs over, the one named last changes fastest.
Arguments:
- queries: bfloat16 [2048, 768], P(('blk', 'rep'), 'head'), may hold values from -400 to 400
- keys: bfloat16 [2048, 256], P(('blk', 'rep'), 'head'), may hold values from -6 to 6
- values: bfloat16 [2048, 256], P(('blk', 'rep'), 'head'), may hold values from -18 to 18
- stretch_order: int32 [16], replicated, may hold values from 0 to 15, each once
- out_weight: bfloat16 [768, 3072], P('head'), may hold values from -0.21875 to 0.21875
Outputs:
- mixed_rows: bfloat16 [2048, 3072], P(('blk', 'rep'), 'head')
- log_sum_exp: float32 [6, 2048], P('head', ('blk', 'rep'))
The draws below stay inside these ranges and needn't reach their ends.
Inputs may be any that keep to these rules, and one draw needn't show every extreme that they name: `stretch_order`: each stretch number appears once.
All inputs are finite; a program needn't handle non-finite values.
Results may differ from the reference program's by a relative error of at most 0.02.
Values may be sent and summed in bfloat16 or wider, within the bound.
No kernel may reach another device: no remote copies, remote signals or barrier semaphores. Data moves between devices by JAX's collectives and lax.ppermute only.
A program may use at most 128 MiB of HBM per device.

```python
import math
import jax
import jax.numpy as jnp
from jax import lax

D = 3072
GROUP = 3
DH = 128
KVH_DEV = 1
TOK_DEV = 128
KV_HEADS = 2
QHEADS = 6
NCHUNKS = 16
SEQ = 2048
N_HEAD = 2


def draw_keys(key, part):
    drawn_keys = jnp.clip(jax.random.normal(jax.random.fold_in(key, 3), (SEQ, KV_HEADS * DH), jnp.float32), -6.0, 6.0)
    return drawn_keys.astype(jnp.bfloat16)


def draw_queries(key, part):
    drawn_queries = jnp.clip(2.0 * jax.random.normal(jax.random.fold_in(key, 5), (SEQ, QHEADS * DH), jnp.float32), -12.0, 12.0)
    return drawn_queries.astype(jnp.bfloat16)


def block_scale(stream_key, extent, pieces, least, top_value):
    def one(axis_at, blocks):
        draws = jax.random.uniform(jax.random.fold_in(jax.random.fold_in(stream_key, 6), axis_at), (blocks,), jnp.float32, least / len(pieces), top_value / len(pieces))
        return jnp.repeat(jnp.exp(draws), extent[axis_at] // blocks).reshape((-1,) + (1,) * (len(extent) - axis_at - 1))

    factor_of = one(*pieces[0])
    for cut in pieces[1:]:
        factor_of = factor_of * one(*cut)
    return factor_of


def normal_values(stream_key, extent, scale, limit, cuts=(), kind=jnp.bfloat16):
    loudness = block_scale(stream_key, extent, cuts, -0.22, 0.18) if cuts else 1.0
    array = jax.random.normal(stream_key, extent, jnp.float32) * scale * loudness
    return jnp.minimum(jnp.maximum(array, -limit), limit).astype(kind)


def setup_inputs(seed: int = 0) -> dict:
    splits = jax.random.split(jax.random.key(seed), 6)
    queries = draw_queries(jax.random.fold_in(splits[5], 71), 0)
    keys = draw_keys(jax.random.fold_in(splits[5], 71), 0)
    values = normal_values(splits[2], (SEQ, KV_HEADS * DH), 3.0, 18.0, ((0, 16), (1, 2)))
    stretch_order = jax.random.permutation(splits[3], NCHUNKS).astype(jnp.int32)
    out_weight = normal_values(splits[4], (QHEADS * DH, D), (QHEADS * DH) ** -0.5, 0.21875, ((0, 2),))
    return dict(queries=queries, keys=keys, values=values, stretch_order=stretch_order, out_weight=out_weight)


def reference(queries, keys, values, stretch_order, out_weight):
    seq_len = queries.shape[0]
    row_ids = jnp.arange(seq_len, dtype=jnp.int32)
    positions = stretch_order[row_ids // TOK_DEV].astype(jnp.int32) * TOK_DEV + row_ids % TOK_DEV
    query_heads = queries.astype(jnp.float32).reshape(seq_len, QHEADS, DH).transpose(1, 0, 2)
    key_heads = keys.astype(jnp.float32).reshape(seq_len, KV_HEADS, DH).transpose(1, 0, 2)
    value_heads = values.astype(jnp.float32).reshape(seq_len, KV_HEADS, DH).transpose(1, 0, 2)
    block_len = math.gcd(seq_len, 1024)
    block_count = seq_len // block_len
    factor = DH ** (-0.5)

    def one_block(flat_index):
        head_index = flat_index // block_count
        block_index = flat_index % block_count
        group_index = head_index // GROUP
        query_head = lax.dynamic_index_in_dim(query_heads, head_index, 0, keepdims=False)
        query_block = lax.dynamic_slice_in_dim(query_head, block_index * block_len, block_len, 0)
        key_head = lax.dynamic_index_in_dim(key_heads, group_index, 0, keepdims=False)
        value_head = lax.dynamic_index_in_dim(value_heads, group_index, 0, keepdims=False)
        query_pos = lax.dynamic_slice_in_dim(positions, block_index * block_len, block_len, 0)
        scores = jnp.dot(query_block, key_head.T, precision=lax.Precision.HIGHEST) * factor
        allowed = positions[None, :] <= query_pos[:, None]
        masked = jnp.where(allowed, scores, -jnp.inf)
        row_top = jnp.max(masked, axis=1)
        expanded = jnp.where(allowed, jnp.exp(scores - row_top[:, None]), 0.0)
        totals = jnp.sum(expanded, axis=1)
        weights = lax.optimization_barrier(expanded.astype(jnp.bfloat16)).astype(jnp.float32)
        attended = jnp.dot(weights, value_head, precision=lax.Precision.HIGHEST) / totals[:, None]
        return (attended.astype(jnp.bfloat16), row_top + jnp.log(totals))
    outputs, sums = lax.map(one_block, jnp.arange(QHEADS * block_count, dtype=jnp.int32))
    attended = outputs.reshape(QHEADS, seq_len, DH).transpose(1, 0, 2).reshape(seq_len, QHEADS * DH)
    log_sum_exp = sums.reshape(QHEADS, seq_len)
    width = KVH_DEV * GROUP * DH
    mixed = jnp.zeros((seq_len, out_weight.shape[1]), jnp.float32)
    for rank in range(N_HEAD):
        partial_value = jnp.dot(attended[:, rank * width:(rank + 1) * width].astype(jnp.float32), out_weight[rank * width:(rank + 1) * width].astype(jnp.float32), precision=lax.Precision.HIGHEST)
        mixed = mixed + lax.optimization_barrier(partial_value.astype(jnp.bfloat16)).astype(jnp.float32)
    return (mixed.astype(jnp.bfloat16), log_sum_exp)
```

```python
import math

import jax
import jax.numpy as jnp
from jax import lax
from jax.experimental import pallas as pl
from jax.experimental.pallas import tpu as pltpu
from jax.sharding import PartitionSpec as P

GROUP = 3
DH = 128
NEG_FILL = -1e30
LOG2E = math.log2(math.e)
STAT_ROWS = 16


VMEM = pl.BlockSpec(memory_space=pltpu.VMEM)
SMEM = pl.BlockSpec(memory_space=pltpu.SMEM)
HBM = pl.BlockSpec(memory_space=pl.ANY)


def source_of(me, hop, count):
    if count & (count - 1) == 0:
        return lax.bitwise_xor(me, jnp.int32(hop))
    return lax.rem(me + (count - hop), count)


def hops_out(hop, count):
    if count & (count - 1) == 0:
        return [(i, i ^ hop) for i in range(count)]
    return [(i, (i + hop) % count) for i in range(count)]


def hops_back(hop, count):
    return [(b, a) for a, b in hops_out(hop, count)]


def pack_kernel(keys_ref, values_ref, packed_ref):
    for head in range(packed_ref.shape[0]):
        cols = slice(head * DH, (head + 1) * DH)
        packed_ref[head, 0] = keys_ref[:, cols]
        packed_ref[head, 1] = values_ref[:, cols].T


def attend_kernel(rep_hop, spans, span_len, order_ref, query_ref, *refs):
    kv_refs, out_ref = refs[:spans], refs[spans]
    blk_rank, rep_rank = lax.axis_index("blk"), lax.axis_index("rep")
    tok = query_ref.shape[0]
    kv_heads = kv_refs[0].shape[0]
    factor = DH**-0.5
    query_pos = order_ref[blk_rank * span_len + source_of(rep_rank, rep_hop, span_len)]
    ahead = lax.broadcasted_iota(jnp.int32, (tok, tok), 0) - lax.broadcasted_iota(
        jnp.int32, (tok, tok), 1
    )
    allowed = []
    for hop in range(spans):
        key_pos = order_ref[source_of(blk_rank, hop, spans) * span_len + rep_rank]
        allowed.append(ahead <= (query_pos - key_pos) * tok)
    for kv_head in range(kv_heads):
        for group in range(GROUP):
            head = kv_head * GROUP + group
            cols = slice(head * DH, (head + 1) * DH)
            rows = slice(head * tok, (head + 1) * tok)
            query = query_ref[:, cols]
            scores = []
            for hop in range(spans):
                raw = lax.dot_general(
                    kv_refs[hop][kv_head, 0],
                    query,
                    (((1,), (1,)), ((), ())),
                    preferred_element_type=jnp.float32,
                )
                scores.append(jnp.where(allowed[hop], raw, NEG_FILL))
            top = scores[0]
            for hop in range(1, spans):
                top = jnp.maximum(top, scores[hop])
            top = jnp.max(top, axis=0, keepdims=True)
            weight_sum = None
            numer = jnp.zeros((DH, tok), jnp.float32)
            for hop in range(spans):
                weights = jnp.exp2((scores[hop] - top) * (factor * LOG2E))
                weight_sum = weights if weight_sum is None else weight_sum + weights
                numer = numer + lax.dot_general(
                    kv_refs[hop][kv_head, 1],
                    weights.astype(jnp.bfloat16),
                    (((1,), (0,)), ((), ())),
                    preferred_element_type=jnp.float32,
                )
            total = jnp.sum(weight_sum, axis=0, keepdims=True)
            out_ref[0:DH, rows] = (numer / total).astype(jnp.bfloat16)
            log_sum = top * factor + jnp.log(total)
            high = log_sum.astype(jnp.bfloat16)
            rest = log_sum - high.astype(jnp.float32)
            middle = rest.astype(jnp.bfloat16)
            low = (rest - middle.astype(jnp.float32)).astype(jnp.bfloat16)
            out_ref[DH : DH + STAT_ROWS, rows] = jnp.concatenate(
                [high, middle, low, jnp.zeros((STAT_ROWS - 3, tok), jnp.bfloat16)], axis=0
            )


def combine_kernel(tok, *refs):
    part_refs, (attended_ref, log_sum_ref) = refs[:-2], refs[-2:]
    stats = []
    for part in part_refs:
        parts = part[DH : DH + STAT_ROWS, :].astype(jnp.float32)
        stats.append(parts[0:1] + parts[1:2] + parts[2:3])
    top = stats[0]
    for stat in stats[1:]:
        top = jnp.maximum(top, stat)
    shares = [jnp.exp(stat - top) for stat in stats]
    total = shares[0]
    for share in shares[1:]:
        total = total + share
    numer = None
    for part, share in zip(part_refs, shares):
        term = part[0:DH, :].astype(jnp.float32) * (share / total)
        numer = term if numer is None else numer + term
    attended_ref[...] = numer.astype(jnp.bfloat16)
    log_sum = top + jnp.log(total)
    for head in range(log_sum_ref.shape[0]):
        log_sum_ref[head : head + 1, :] = log_sum[:, head * tok : (head + 1) * tok]


def project(attended_ref, weight, tok):
    out = None
    for head in range(weight.shape[0] // DH):
        term = lax.dot_general(
            attended_ref[:, head * tok : (head + 1) * tok],
            weight[head * DH : (head + 1) * DH, :],
            (((0,), (0,)), ((), ())),
            preferred_element_type=jnp.float32,
        )
        out = term if out is None else out + term
    return out.astype(jnp.bfloat16)


def project_away_kernel(attended_ref, weight_ref, out_ref):
    tok, width = out_ref.shape
    start = pl.multiple_of((1 - lax.axis_index("head")) * width, 128)
    out_ref[...] = project(attended_ref, weight_ref[:, pl.ds(start, width)], tok)


def project_home_kernel(attended_ref, weight_ref, other_ref, out_ref):
    tok, width = out_ref.shape
    start = pl.multiple_of(lax.axis_index("head") * width, 128)
    mine = project(attended_ref, weight_ref[:, pl.ds(start, width)], tok)
    out_ref[...] = (
        mine.astype(jnp.float32) + other_ref[...].astype(jnp.float32)
    ).astype(jnp.bfloat16)


def params(mib):
    return pltpu.CompilerParams(vmem_limit_bytes=mib * 2**20)


def cost(flops, moved, transcendentals=0):
    return pl.CostEstimate(flops=flops, bytes_accessed=moved, transcendentals=transcendentals)


def body(queries, keys, values, stretch_order, out_weight):
    tok = queries.shape[0]
    kv_heads = keys.shape[1] // DH
    heads = kv_heads * GROUP
    width = out_weight.shape[1] // lax.axis_size("head")
    spans, span_len = lax.axis_size("blk"), lax.axis_size("rep")
    packed = pl.pallas_call(
        pack_kernel,
        out_shape=jax.ShapeDtypeStruct((kv_heads, 2, tok, DH), jnp.bfloat16),
        in_specs=[VMEM, VMEM],
        out_specs=VMEM,
        name="pack",
        compiler_params=params(4),
    )(keys, values)
    kv = [packed] + [
        lax.ppermute(packed, "blk", hops_out(hop, spans)) for hop in range(1, spans)
    ]
    query = [queries] + [
        lax.ppermute(queries, "rep", hops_out(hop, span_len)) for hop in range(1, span_len)
    ]
    parts = []
    for hop in range(span_len):
        parts.append(
            pl.pallas_call(
                lambda *refs, hop=hop: attend_kernel(hop, spans, span_len, *refs),
                out_shape=jax.ShapeDtypeStruct((DH + STAT_ROWS, heads * tok), jnp.bfloat16),
                in_specs=[SMEM] + [VMEM] * (1 + spans),
                out_specs=VMEM,
                cost_estimate=cost(
                    4 * heads * tok * spans * tok * DH,
                    2 * heads * tok * DH * 2 + spans * tok * DH * 4,
                    heads * tok * spans * tok,
                ),
                name="attend",
                compiler_params=params(8),
            )(stretch_order, query[hop], *kv)
        )
    returned = [parts[0]] + [
        lax.ppermute(parts[hop], "rep", hops_back(hop, span_len)) for hop in range(1, span_len)
    ]
    attended, log_sum = pl.pallas_call(
        lambda *refs: combine_kernel(tok, *refs),
        out_shape=(
            jax.ShapeDtypeStruct((DH, heads * tok), jnp.bfloat16),
            jax.ShapeDtypeStruct((heads, tok), jnp.float32),
        ),
        in_specs=[VMEM] * span_len,
        out_specs=(VMEM, VMEM),
        name="combine",
        compiler_params=params(4),
    )(*returned)
    shape = jax.ShapeDtypeStruct((tok, width), jnp.bfloat16)
    project_cost = cost(2 * tok * heads * DH * width, heads * DH * width * 2)
    away = pl.pallas_call(
        project_away_kernel,
        out_shape=shape,
        in_specs=[VMEM, VMEM],
        out_specs=VMEM,
        cost_estimate=project_cost,
        name="project_away",
        compiler_params=params(12),
    )(attended, out_weight)
    other = lax.ppermute(away, "head", [(0, 1), (1, 0)])
    mixed_rows = pl.pallas_call(
        project_home_kernel,
        out_shape=shape,
        in_specs=[VMEM, VMEM, VMEM],
        out_specs=VMEM,
        cost_estimate=project_cost,
        name="project_home",
        compiler_params=params(12),
    )(attended, out_weight, other)
    return (mixed_rows, log_sum)


def solution(mesh):
    in_specs = (
        P(("blk", "rep"), "head"),
        P(("blk", "rep"), "head"),
        P(("blk", "rep"), "head"),
        P(),
        P("head", None),
    )
    out_specs = (P(("blk", "rep"), "head"), P("head", ("blk", "rep")))
    return jax.shard_map(body, mesh=mesh, in_specs=in_specs, out_specs=out_specs, check_vma=False)
```

```python
import math

import jax
import jax.numpy as jnp
from jax import lax
from jax.experimental import pallas as pl
from jax.experimental.pallas import tpu as pltpu
from jax.sharding import PartitionSpec as P


GROUP = 3
DH = 128
NEG_FILL = -1e30
LOG2E = math.log2(math.e)
STAT_ROWS = 16


VMEM = pl.BlockSpec(memory_space=pltpu.VMEM)
HBM = pl.BlockSpec(memory_space=pltpu.HBM)


def source_of(me, hop, count):
    if count & (count - 1) == 0:
        return lax.bitwise_xor(me, jnp.int32(hop))
    return lax.rem(me + (count - hop), count)


def hops_out(hop, count):
    if count & (count - 1) == 0:
        return [(i, i ^ hop) for i in range(count)]
    return [(i, (i + hop) % count) for i in range(count)]


def hops_back(hop, count):
    return [(b, a) for a, b in hops_out(hop, count)]


def pack_kernel(
    spans, span_len, query_hbm, keys_hbm, values_hbm, order_hbm,
    query_ref, packed_ref, bound_ref, values_ref, order_ref, sems,
):
    tok = values_ref.shape[0]
    heads, kv_heads = query_ref.shape[0] // tok, packed_ref.shape[0]
    order_copy = pltpu.make_async_copy(order_hbm, order_ref, sems.at[0])
    value_copy = pltpu.make_async_copy(values_hbm, values_ref, sems.at[1])
    copies = []
    for head in range(kv_heads):
        copies.append((keys_hbm.at[:, pl.ds(head * DH, DH)], packed_ref.at[head, 0]))
    for head in range(heads):
        copies.append(
            (query_hbm.at[:, pl.ds(head * DH, DH)], query_ref.at[pl.ds(head * tok, tok), :])
        )
    copies = [
        pltpu.make_async_copy(source, target, sems.at[2 + at])
        for at, (source, target) in enumerate(copies)
    ]
    value_copy.start()
    order_copy.start()
    for copy in copies:
        copy.start()
    value_copy.wait()
    for head in range(kv_heads):
        packed_ref[head, 1] = values_ref[:, head * DH : (head + 1) * DH].T
    order_copy.wait()
    blk_rank, rep_rank = lax.axis_index("blk"), lax.axis_index("rep")
    for rep_hop in range(span_len):
        query_at = blk_rank * span_len + source_of(rep_rank, rep_hop, span_len)
        for hop in range(spans):
            key_at = source_of(blk_rank, hop, spans) * span_len + rep_rank
            row = rep_hop * spans + hop
            bound_ref[row : row + 1, :] = jnp.full(
                (1, tok), (order_ref[query_at] - order_ref[key_at]) * tok, jnp.int32
            )
    for copy in copies:
        copy.wait()


def piece_start(piece, pieces, piece_width):
    half = pieces // 2
    head = lax.axis_index("head")
    block = 1 - head if piece < half else head
    return (block * half + piece % half) * piece_width


def attend_kernel(rep_hop, spans, span_len, bound_ref, query_ref, *refs):
    kv_refs, (weight_hbm, out_ref, piece_ref, sem) = refs[:spans], refs[spans:]
    columns = piece_start(rep_hop, span_len, piece_ref.shape[1])
    fetch = pltpu.make_async_copy(
        weight_hbm.at[:, pl.ds(pl.multiple_of(columns, 128), piece_ref.shape[1])], piece_ref, sem
    )
    fetch.start()
    tok = bound_ref.shape[1]
    kv_heads = kv_refs[0].shape[0]
    factor = DH**-0.5
    lanes = GROUP * tok
    ahead = lax.broadcasted_iota(jnp.int32, (tok, tok), 0) - lax.broadcasted_iota(
        jnp.int32, (tok, tok), 1
    )
    ahead = jnp.concatenate([ahead] * GROUP, axis=1)
    for kv_head in range(kv_heads):
        rows = slice(kv_head * lanes, (kv_head + 1) * lanes)
        query = query_ref[rows, :]
        scores = []
        for hop in range(spans):
            raw = lax.dot_general(
                kv_refs[hop][kv_head, 0],
                query,
                (((1,), (1,)), ((), ())),
                preferred_element_type=jnp.float32,
            )
            at = rep_hop * spans + hop
            bound = jnp.concatenate([bound_ref[at : at + 1, :]] * GROUP, axis=1)
            scores.append(jnp.where(ahead <= bound, raw, NEG_FILL))
        top = scores[0]
        for hop in range(1, spans):
            top = jnp.maximum(top, scores[hop])
        top = jnp.max(top, axis=0, keepdims=True)
        weight_sum, numer = None, None
        for hop in range(spans):
            weights = jnp.exp2((scores[hop] - top) * (factor * LOG2E))
            weight_sum = weights if weight_sum is None else weight_sum + weights
            term = lax.dot_general(
                kv_refs[hop][kv_head, 1],
                weights.astype(jnp.bfloat16),
                (((1,), (0,)), ((), ())),
                preferred_element_type=jnp.float32,
            )
            numer = term if numer is None else numer + term
        total = jnp.sum(weight_sum, axis=0, keepdims=True)
        out_ref[0:DH, rows] = (numer * (1.0 / total)).astype(jnp.bfloat16)
        log_sum = top * factor + jnp.log(total)
        high = log_sum.astype(jnp.bfloat16)
        rest = log_sum - high.astype(jnp.float32)
        middle = rest.astype(jnp.bfloat16)
        low = (rest - middle.astype(jnp.float32)).astype(jnp.bfloat16)
        out_ref[DH : DH + STAT_ROWS, rows] = jnp.concatenate(
            [high, middle, low, jnp.zeros((STAT_ROWS - 3, lanes), jnp.bfloat16)], axis=0
        )
    fetch.wait()


def combine_project_kernel(part_count, *refs):
    part_refs, weight_refs = refs[:part_count], refs[part_count:-3]
    away_ref, attended_ref, log_sum_ref = refs[-3:]
    stats = []
    for part in part_refs:
        parts = part[DH : DH + STAT_ROWS, :].astype(jnp.float32)
        stats.append(parts[0:1] + parts[1:2] + parts[2:3])
    top = stats[0]
    for stat in stats[1:]:
        top = jnp.maximum(top, stat)
    shares = [jnp.exp(stat - top) for stat in stats]
    total = shares[0]
    for share in shares[1:]:
        total = total + share
    scale = 1.0 / total
    numer = None
    for part, share in zip(part_refs, shares):
        term = part[0:DH, :].astype(jnp.float32) * (share * scale)
        numer = term if numer is None else numer + term
    attended = numer.astype(jnp.bfloat16)
    attended_ref[...] = attended
    log_sum_ref[...] = jnp.broadcast_to(top + jnp.log(total), log_sum_ref.shape)
    project(attended, weight_refs, away_ref)


def project(attended, weight_refs, out_ref):
    tok, piece_width = out_ref.shape[0], weight_refs[0].shape[1]
    for piece, weight_ref in enumerate(weight_refs):
        out = None
        for head in range(weight_ref.shape[0] // DH):
            term = lax.dot_general(
                attended[:, head * tok : (head + 1) * tok],
                weight_ref[head * DH : (head + 1) * DH, :],
                (((0,), (0,)), ((), ())),
                preferred_element_type=jnp.float32,
            )
            out = term if out is None else out + term
        columns = slice(piece * piece_width, (piece + 1) * piece_width)
        out_ref[:, columns] = out.astype(jnp.bfloat16)


def project_home_kernel(attended_ref, *refs):
    project(attended_ref[...], refs[:-1], refs[-1])


def add_kernel(home_ref, other_ref, log_row_ref, out_ref, log_sum_ref):
    tok = out_ref.shape[0]
    out_ref[...] = (
        home_ref[...].astype(jnp.float32) + other_ref[...].astype(jnp.float32)
    ).astype(jnp.bfloat16)
    for head in range(log_sum_ref.shape[0]):
        log_sum_ref[head : head + 1, :] = log_row_ref[0:1, head * tok : (head + 1) * tok]


def cost(flops, moved, transcendentals=0):
    return pl.CostEstimate(flops=flops, bytes_accessed=moved, transcendentals=transcendentals)


def in_hbm(array):
    return pltpu.with_memory_space_constraint(array, pltpu.HBM)


def params(mib):
    return pltpu.CompilerParams(vmem_limit_bytes=mib * 2**20)


def body(queries, keys, values, stretch_order, out_weight):
    tok = queries.shape[0]
    kv_heads = keys.shape[1] // DH
    heads = kv_heads * GROUP
    width = out_weight.shape[1] // lax.axis_size("head")
    spans, span_len = lax.axis_size("blk"), lax.axis_size("rep")
    query, packed, bounds = pl.pallas_call(
        lambda *refs: pack_kernel(spans, span_len, *refs),
        out_shape=(
            jax.ShapeDtypeStruct((heads * tok, DH), jnp.bfloat16),
            jax.ShapeDtypeStruct((kv_heads, 2, tok, DH), jnp.bfloat16),
            jax.ShapeDtypeStruct((spans * span_len, tok), jnp.int32),
        ),
        in_specs=[HBM] * 4,
        out_specs=(VMEM, VMEM, VMEM),
        scratch_shapes=[
            pltpu.VMEM((tok, kv_heads * DH), jnp.bfloat16),
            pltpu.SMEM(stretch_order.shape, jnp.int32),
            pltpu.SemaphoreType.DMA((2 + kv_heads + heads,)),
        ],
        compiler_params=params(4),
        name="pack",
    )(*[in_hbm(x) for x in (queries, keys, values, stretch_order)])
    kv, query = [packed], [query]
    for hop in range(1, spans):
        kv.append(lax.ppermute(packed, "blk", hops_out(hop, spans)))
    for hop in range(1, span_len):
        query.append(lax.ppermute(query[0], "rep", hops_out(hop, span_len)))
    parts, pieces = [], []
    piece_width = out_weight.shape[1] // span_len
    for hop in range(span_len):
        part, piece = pl.pallas_call(
            lambda *refs, hop=hop: attend_kernel(hop, spans, span_len, *refs),
            out_shape=(
                jax.ShapeDtypeStruct((DH + STAT_ROWS, heads * tok), jnp.bfloat16),
                jax.ShapeDtypeStruct((heads * DH, piece_width), jnp.bfloat16),
            ),
            in_specs=[VMEM] * (2 + spans) + [HBM],
            out_specs=(VMEM, VMEM),
            scratch_shapes=[pltpu.SemaphoreType.DMA],
            cost_estimate=cost(
                4 * heads * tok * spans * tok * DH,
                2 * heads * tok * DH * 2 + spans * tok * DH * 4 + heads * DH * piece_width * 4,
                heads * tok * spans * tok,
            ),
            compiler_params=params(16 if spans > 8 else 8),
            name="attend",
        )(bounds, query[hop], *kv, in_hbm(out_weight))
        parts.append(part)
        pieces.append(piece)
    returned = [parts[0]]
    for hop in range(1, span_len):
        returned.append(lax.ppermute(parts[hop], "rep", hops_back(hop, span_len)))
    shape = jax.ShapeDtypeStruct((tok, width), jnp.bfloat16)
    project_cost = cost(2 * tok * heads * DH * width, heads * DH * width * 2)
    half = span_len // 2
    away, attended, log_row = pl.pallas_call(
        lambda *refs: combine_project_kernel(span_len, *refs),
        out_shape=(
            shape,
            jax.ShapeDtypeStruct((DH, heads * tok), jnp.bfloat16),
            jax.ShapeDtypeStruct((8, heads * tok), jnp.float32),
        ),
        in_specs=[VMEM] * (span_len + half),
        out_specs=(VMEM, VMEM, VMEM),
        cost_estimate=project_cost,
        compiler_params=params(8),
        name="combine_project",
    )(*returned, *pieces[:half])
    other = lax.ppermute(away, "head", [(0, 1), (1, 0)])
    home = pl.pallas_call(
        project_home_kernel,
        out_shape=shape,
        in_specs=[VMEM] * (1 + half),
        out_specs=VMEM,
        cost_estimate=project_cost,
        compiler_params=params(8),
        name="project_home",
    )(attended, *pieces[half:])
    return pl.pallas_call(
        add_kernel,
        out_shape=(shape, jax.ShapeDtypeStruct((heads, tok), jnp.float32)),
        in_specs=[VMEM, VMEM, VMEM],
        out_specs=(VMEM, VMEM),
        compiler_params=params(4),
        name="add",
    )(home, other, log_row)


def solution(mesh):
    in_specs = (
        P(("blk", "rep"), "head"),
        P(("blk", "rep"), "head"),
        P(("blk", "rep"), "head"),
        P(),
        P("head", None),
    )
    out_specs = (P(("blk", "rep"), "head"), P("head", ("blk", "rep")))

    return jax.shard_map(body, mesh=mesh, in_specs=in_specs, out_specs=out_specs, check_vma=False)
```

```python
import math

import jax
import jax.numpy as jnp
from jax import lax
from jax.experimental import pallas as pl
from jax.experimental.pallas import tpu as pltpu
from jax.sharding import PartitionSpec as P


GROUP = 3
DH = 128
NEG_FILL = -1e30
LOG2E = math.log2(math.e)
STAT_ROWS = 16


VMEM = pl.BlockSpec(memory_space=pltpu.VMEM)
HBM = pl.BlockSpec(memory_space=pltpu.HBM)


def source_of(me, hop, count):
    if count & (count - 1) == 0:
        return lax.bitwise_xor(me, jnp.int32(hop))
    return lax.rem(me + (count - hop), count)


def hops_out(hop, count):
    if count & (count - 1) == 0:
        return [(i, i ^ hop) for i in range(count)]
    return [(i, (i + hop) % count) for i in range(count)]


def hops_back(hop, count):
    return [(b, a) for a, b in hops_out(hop, count)]


def pack_kernel(
    spans, span_len, query_hbm, keys_hbm, values_hbm, order_hbm,
    query_ref, packed_ref, bound_ref, values_ref, order_ref, sems,
):
    tok = values_ref.shape[0]
    heads, kv_heads = query_ref.shape[0] // tok, packed_ref.shape[0]
    order_copy = pltpu.make_async_copy(order_hbm, order_ref, sems.at[0])
    value_copy = pltpu.make_async_copy(values_hbm, values_ref, sems.at[1])
    copies = []
    for head in range(kv_heads):
        copies.append((keys_hbm.at[:, pl.ds(head * DH, DH)], packed_ref.at[head, 0]))
    for head in range(heads):
        copies.append(
            (query_hbm.at[:, pl.ds(head * DH, DH)], query_ref.at[pl.ds(head * tok, tok), :])
        )
    copies = [
        pltpu.make_async_copy(source, target, sems.at[2 + at])
        for at, (source, target) in enumerate(copies)
    ]
    value_copy.start()
    order_copy.start()
    for copy in copies:
        copy.start()
    value_copy.wait()
    for head in range(kv_heads):
        packed_ref[head, 1] = values_ref[:, head * DH : (head + 1) * DH].T
    order_copy.wait()
    blk_rank, rep_rank = lax.axis_index("blk"), lax.axis_index("rep")
    for rep_hop in range(span_len):
        query_at = blk_rank * span_len + source_of(rep_rank, rep_hop, span_len)
        for hop in range(spans):
            key_at = source_of(blk_rank, hop, spans) * span_len + rep_rank
            row = rep_hop * spans + hop
            bound_ref[row : row + 1, :] = jnp.full(
                (1, tok), (order_ref[query_at] - order_ref[key_at]) * tok, jnp.int32
            )
    for copy in copies:
        copy.wait()


def attend_kernel(rep_hop, spans, bound_ref, query_ref, *refs):
    kv_refs, out_ref = refs[:spans], refs[spans]
    tok = bound_ref.shape[1]
    kv_heads = kv_refs[0].shape[0]
    factor = DH**-0.5
    lanes = GROUP * tok
    ahead = lax.broadcasted_iota(jnp.int32, (tok, tok), 0) - lax.broadcasted_iota(
        jnp.int32, (tok, tok), 1
    )
    ahead = jnp.concatenate([ahead] * GROUP, axis=1)
    for kv_head in range(kv_heads):
        rows = slice(kv_head * lanes, (kv_head + 1) * lanes)
        query = query_ref[rows, :]
        scores = []
        for hop in range(spans):
            raw = lax.dot_general(
                kv_refs[hop][kv_head, 0],
                query,
                (((1,), (1,)), ((), ())),
                preferred_element_type=jnp.float32,
            )
            at = rep_hop * spans + hop
            bound = jnp.concatenate([bound_ref[at : at + 1, :]] * GROUP, axis=1)
            scores.append(jnp.where(ahead <= bound, raw, NEG_FILL))
        top = scores[0]
        for hop in range(1, spans):
            top = jnp.maximum(top, scores[hop])
        top = jnp.max(top, axis=0, keepdims=True)
        weight_sum, numer = None, None
        for hop in range(spans):
            weights = jnp.exp2((scores[hop] - top) * (factor * LOG2E))
            weight_sum = weights if weight_sum is None else weight_sum + weights
            term = lax.dot_general(
                kv_refs[hop][kv_head, 1],
                weights.astype(jnp.bfloat16),
                (((1,), (0,)), ((), ())),
                preferred_element_type=jnp.float32,
            )
            numer = term if numer is None else numer + term
        total = jnp.sum(weight_sum, axis=0, keepdims=True)
        out_ref[0:DH, rows] = (numer * (1.0 / total)).astype(jnp.bfloat16)
        log_sum = top * factor + jnp.log(total)
        high = log_sum.astype(jnp.bfloat16)
        rest = log_sum - high.astype(jnp.float32)
        middle = rest.astype(jnp.bfloat16)
        low = (rest - middle.astype(jnp.float32)).astype(jnp.bfloat16)
        out_ref[DH : DH + STAT_ROWS, rows] = jnp.concatenate(
            [high, middle, low, jnp.zeros((STAT_ROWS - 3, lanes), jnp.bfloat16)], axis=0
        )


def attend_fetch_kernel(spans, chunks, *refs):
    weight_hbm, part_ref, weight_ref, sems = refs[-4:]
    rows = weight_ref.shape[0] // chunks
    copies = []
    for chunk in range(chunks):
        here = pl.ds(chunk * rows, rows)
        copies.append(
            pltpu.make_async_copy(weight_hbm.at[here, :], weight_ref.at[here, :], sems.at[chunk])
        )
        copies[-1].start()
    attend_kernel(0, spans, *refs[:-4], part_ref)
    for copy in copies:
        copy.wait()


def combine_project_kernel(part_count, *refs):
    part_refs, weight_ref = refs[:part_count], refs[part_count]
    away_ref, attended_ref, log_sum_ref = refs[-3:]
    stats = []
    for part in part_refs:
        parts = part[DH : DH + STAT_ROWS, :].astype(jnp.float32)
        stats.append(parts[0:1] + parts[1:2] + parts[2:3])
    top = stats[0]
    for stat in stats[1:]:
        top = jnp.maximum(top, stat)
    shares = [jnp.exp(stat - top) for stat in stats]
    total = shares[0]
    for share in shares[1:]:
        total = total + share
    scale = 1.0 / total
    numer = None
    for part, share in zip(part_refs, shares):
        term = part[0:DH, :].astype(jnp.float32) * (share * scale)
        numer = term if numer is None else numer + term
    attended = numer.astype(jnp.bfloat16)
    attended_ref[...] = attended
    log_sum_ref[...] = jnp.broadcast_to(top + jnp.log(total), log_sum_ref.shape)
    project(attended, weight_ref, 1 - lax.axis_index("head"), away_ref)


def project(attended, weight_ref, block, out_ref):
    tok, width = out_ref.shape
    columns = pl.ds(pl.multiple_of(block * width, 128), width)
    out = None
    for head in range(weight_ref.shape[0] // DH):
        term = lax.dot_general(
            attended[:, head * tok : (head + 1) * tok],
            weight_ref[head * DH : (head + 1) * DH, columns],
            (((0,), (0,)), ((), ())),
            preferred_element_type=jnp.float32,
        )
        out = term if out is None else out + term
    out_ref[...] = out.astype(jnp.bfloat16)


def project_home_kernel(attended_ref, weight_ref, out_ref):
    project(attended_ref[...], weight_ref, lax.axis_index("head"), out_ref)


def add_kernel(home_ref, other_ref, log_row_ref, out_ref, log_sum_ref):
    tok = out_ref.shape[0]
    out_ref[...] = (
        home_ref[...].astype(jnp.float32) + other_ref[...].astype(jnp.float32)
    ).astype(jnp.bfloat16)
    for head in range(log_sum_ref.shape[0]):
        log_sum_ref[head : head + 1, :] = log_row_ref[0:1, head * tok : (head + 1) * tok]


def cost(flops, moved, transcendentals=0):
    return pl.CostEstimate(flops=flops, bytes_accessed=moved, transcendentals=transcendentals)


def in_hbm(array):
    return pltpu.with_memory_space_constraint(array, pltpu.HBM)


def params(mib):
    return pltpu.CompilerParams(vmem_limit_bytes=mib * 2**20)


def body(queries, keys, values, stretch_order, out_weight):
    tok = queries.shape[0]
    kv_heads = keys.shape[1] // DH
    heads = kv_heads * GROUP
    width = out_weight.shape[1] // lax.axis_size("head")
    spans, span_len = lax.axis_size("blk"), lax.axis_size("rep")
    query, packed, bounds = pl.pallas_call(
        lambda *refs: pack_kernel(spans, span_len, *refs),
        out_shape=(
            jax.ShapeDtypeStruct((heads * tok, DH), jnp.bfloat16),
            jax.ShapeDtypeStruct((kv_heads, 2, tok, DH), jnp.bfloat16),
            jax.ShapeDtypeStruct((spans * span_len, tok), jnp.int32),
        ),
        in_specs=[HBM] * 4,
        out_specs=(VMEM, VMEM, VMEM),
        scratch_shapes=[
            pltpu.VMEM((tok, kv_heads * DH), jnp.bfloat16),
            pltpu.SMEM(stretch_order.shape, jnp.int32),
            pltpu.SemaphoreType.DMA((2 + kv_heads + heads,)),
        ],
        compiler_params=params(4),
        name="pack",
    )(*[in_hbm(x) for x in (queries, keys, values, stretch_order)])
    kv, query = [packed], [query]
    for hop in range(1, spans):
        kv.append(lax.ppermute(packed, "blk", hops_out(hop, spans)))
    for hop in range(1, span_len):
        query.append(lax.ppermute(query[0], "rep", hops_out(hop, span_len)))
    part_shape = jax.ShapeDtypeStruct((DH + STAT_ROWS, heads * tok), jnp.bfloat16)
    attend = dict(
        cost_estimate=cost(
            4 * heads * tok * spans * tok * DH,
            2 * heads * tok * DH * 2 + spans * tok * DH * 4,
            heads * tok * spans * tok,
        ),
        compiler_params=params(16 if spans > 8 else 8),
    )
    chunks = heads * DH // math.gcd(heads * DH, 64)
    parts = [None]
    for hop in range(1, span_len):
        parts.append(
            pl.pallas_call(
                lambda *refs, hop=hop: attend_kernel(hop, spans, *refs),
                out_shape=part_shape,
                in_specs=[VMEM] * (2 + spans),
                out_specs=VMEM,
                name="attend",
                **attend,
            )(bounds, query[hop], *kv)
        )
    parts[0], weight = pl.pallas_call(
        lambda *refs: attend_fetch_kernel(spans, chunks, *refs),
        out_shape=(part_shape, jax.ShapeDtypeStruct(out_weight.shape, jnp.bfloat16)),
        in_specs=[VMEM] * (2 + spans) + [HBM],
        out_specs=(VMEM, VMEM),
        scratch_shapes=[pltpu.SemaphoreType.DMA((chunks,))],
        name="attend_fetch",
        **attend,
    )(bounds, query[0], *kv, in_hbm(out_weight))
    returned = [parts[0]]
    for hop in range(1, span_len):
        returned.append(lax.ppermute(parts[hop], "rep", hops_back(hop, span_len)))
    shape = jax.ShapeDtypeStruct((tok, width), jnp.bfloat16)
    project_cost = cost(2 * tok * heads * DH * width, heads * DH * width * 2)
    away, attended, log_row = pl.pallas_call(
        lambda *refs: combine_project_kernel(span_len, *refs),
        out_shape=(
            shape,
            jax.ShapeDtypeStruct((DH, heads * tok), jnp.bfloat16),
            jax.ShapeDtypeStruct((8, heads * tok), jnp.float32),
        ),
        in_specs=[VMEM] * (span_len + 1),
        out_specs=(VMEM, VMEM, VMEM),
        cost_estimate=project_cost,
        compiler_params=params(8),
        name="combine_project",
    )(*returned, weight)
    other = lax.ppermute(away, "head", [(0, 1), (1, 0)])
    home = pl.pallas_call(
        project_home_kernel,
        out_shape=shape,
        in_specs=[VMEM, VMEM],
        out_specs=VMEM,
        cost_estimate=project_cost,
        compiler_params=params(8),
        name="project_home",
    )(attended, weight)
    return pl.pallas_call(
        add_kernel,
        out_shape=(shape, jax.ShapeDtypeStruct((heads, tok), jnp.float32)),
        in_specs=[VMEM, VMEM, VMEM],
        out_specs=(VMEM, VMEM),
        compiler_params=params(4),
        name="add",
    )(home, other, log_row)


def solution(mesh):
    in_specs = (
        P(("blk", "rep"), "head"),
        P(("blk", "rep"), "head"),
        P(("blk", "rep"), "head"),
        P(),
        P("head", None),
    )
    out_specs = (P(("blk", "rep"), "head"), P("head", ("blk", "rep")))

    return jax.shard_map(body, mesh=mesh, in_specs=in_specs, out_specs=out_specs, check_vma=False)
```

```python
import math

import jax
import jax.numpy as jnp
from jax import lax
from jax.experimental import pallas as pl
from jax.experimental.pallas import tpu as pltpu
from jax.sharding import PartitionSpec as P


GROUP = 3
DH = 128
NEG_FILL = -1e30
LOG2E = math.log2(math.e)
STAT_ROWS = 16
OUT_STEP = 512


VMEM = pl.BlockSpec(memory_space=pltpu.VMEM)
HBM = pl.BlockSpec(memory_space=pltpu.HBM)


def source_of(me, hop, count):
    if count & (count - 1) == 0:
        return lax.bitwise_xor(me, jnp.int32(hop))
    return lax.rem(me + (count - hop), count)


def hops_out(hop, count):
    if count & (count - 1) == 0:
        return [(i, i ^ hop) for i in range(count)]
    return [(i, (i + hop) % count) for i in range(count)]


def hops_back(hop, count):
    return [(b, a) for a, b in hops_out(hop, count)]


def pack_kernel(
    spans, span_len, query_hbm, keys_hbm, values_hbm, order_hbm,
    query_ref, packed_ref, bound_ref, values_ref, order_ref, sems,
):
    tok = values_ref.shape[0]
    heads, kv_heads = query_ref.shape[0] // tok, packed_ref.shape[0]
    order_copy = pltpu.make_async_copy(order_hbm, order_ref, sems.at[0])
    value_copy = pltpu.make_async_copy(values_hbm, values_ref, sems.at[1])
    copies = []
    for head in range(kv_heads):
        copies.append((keys_hbm.at[:, pl.ds(head * DH, DH)], packed_ref.at[head, 0]))
    for head in range(heads):
        copies.append(
            (query_hbm.at[:, pl.ds(head * DH, DH)], query_ref.at[pl.ds(head * tok, tok), :])
        )
    copies = [
        pltpu.make_async_copy(source, target, sems.at[2 + at])
        for at, (source, target) in enumerate(copies)
    ]
    value_copy.start()
    order_copy.start()
    for copy in copies:
        copy.start()
    value_copy.wait()
    for head in range(kv_heads):
        packed_ref[head, 1] = values_ref[:, head * DH : (head + 1) * DH].T
    order_copy.wait()
    blk_rank, rep_rank = lax.axis_index("blk"), lax.axis_index("rep")
    for rep_hop in range(span_len):
        query_at = blk_rank * span_len + source_of(rep_rank, rep_hop, span_len)
        for hop in range(spans):
            key_at = source_of(blk_rank, hop, spans) * span_len + rep_rank
            row = rep_hop * spans + hop
            bound_ref[row : row + 1, :] = jnp.full(
                (1, tok), (order_ref[query_at] - order_ref[key_at]) * tok, jnp.int32
            )
    for copy in copies:
        copy.wait()


def attend_kernel(rep_hop, spans, bound_ref, query_ref, *refs):
    kv_refs, out_ref = refs[:spans], refs[spans]
    tok = bound_ref.shape[1]
    kv_heads = kv_refs[0].shape[0]
    factor = DH**-0.5
    lanes = GROUP * tok
    ahead = lax.broadcasted_iota(jnp.int32, (tok, tok), 0) - lax.broadcasted_iota(
        jnp.int32, (tok, tok), 1
    )
    ahead = jnp.concatenate([ahead] * GROUP, axis=1)
    for kv_head in range(kv_heads):
        rows = slice(kv_head * lanes, (kv_head + 1) * lanes)
        query = query_ref[rows, :]
        scores = []
        for hop in range(spans):
            raw = lax.dot_general(
                kv_refs[hop][kv_head, 0],
                query,
                (((1,), (1,)), ((), ())),
                preferred_element_type=jnp.float32,
            )
            at = rep_hop * spans + hop
            bound = jnp.concatenate([bound_ref[at : at + 1, :]] * GROUP, axis=1)
            scores.append(jnp.where(ahead <= bound, raw, NEG_FILL))
        top = scores[0]
        for hop in range(1, spans):
            top = jnp.maximum(top, scores[hop])
        top = jnp.max(top, axis=0, keepdims=True)
        weight_sum, numer = None, None
        for hop in range(spans):
            weights = jnp.exp2((scores[hop] - top) * (factor * LOG2E))
            weight_sum = weights if weight_sum is None else weight_sum + weights
            term = lax.dot_general(
                kv_refs[hop][kv_head, 1],
                weights.astype(jnp.bfloat16),
                (((1,), (0,)), ((), ())),
                preferred_element_type=jnp.float32,
            )
            numer = term if numer is None else numer + term
        total = jnp.sum(weight_sum, axis=0, keepdims=True)
        out_ref[0:DH, rows] = (numer * (1.0 / total)).astype(jnp.bfloat16)
        log_sum = top * factor + jnp.log(total)
        high = log_sum.astype(jnp.bfloat16)
        rest = log_sum - high.astype(jnp.float32)
        middle = rest.astype(jnp.bfloat16)
        low = (rest - middle.astype(jnp.float32)).astype(jnp.bfloat16)
        out_ref[DH : DH + STAT_ROWS, rows] = jnp.concatenate(
            [high, middle, low, jnp.zeros((STAT_ROWS - 3, lanes), jnp.bfloat16)], axis=0
        )


def attend_fetch_kernel(spans, chunks, *refs):
    weight_hbm, part_ref, weight_ref, sems = refs[-4:]
    rows, width = weight_ref.shape[0] // chunks, weight_ref.shape[1]
    columns = pl.ds(pl.multiple_of(lax.axis_index("head") * width, 128), width)
    copies = []
    for chunk in range(chunks):
        here = pl.ds(chunk * rows, rows)
        copies.append(
            pltpu.make_async_copy(
                weight_hbm.at[here, columns], weight_ref.at[here, :], sems.at[chunk]
            )
        )
        copies[-1].start()
    attend_kernel(0, spans, *refs[:-4], part_ref)
    for copy in copies:
        copy.wait()


def combine_kernel(*refs):
    part_refs, (attended_ref, log_sum_ref) = refs[:-2], refs[-2:]
    stats = []
    for part in part_refs:
        parts = part[DH : DH + STAT_ROWS, :].astype(jnp.float32)
        stats.append(parts[0:1] + parts[1:2] + parts[2:3])
    top = stats[0]
    for stat in stats[1:]:
        top = jnp.maximum(top, stat)
    shares = [jnp.exp(stat - top) for stat in stats]
    total = shares[0]
    for share in shares[1:]:
        total = total + share
    scale = 1.0 / total
    numer = None
    for part, share in zip(part_refs, shares):
        term = part[0:DH, :].astype(jnp.float32) * (share * scale)
        numer = term if numer is None else numer + term
    attended_ref[...] = numer.astype(jnp.bfloat16)
    log_sum = top + jnp.log(total)
    tok = log_sum_ref.shape[1]
    for head in range(log_sum_ref.shape[0]):
        log_sum_ref[head : head + 1, :] = log_sum[:, head * tok : (head + 1) * tok]


def project(attended_ref, weight_ref, tok, columns):
    out = None
    for head in range(weight_ref.shape[0] // DH):
        term = lax.dot_general(
            attended_ref[:, head * tok : (head + 1) * tok],
            weight_ref[head * DH : (head + 1) * DH, columns],
            (((0,), (0,)), ((), ())),
            preferred_element_type=jnp.float32,
        )
        out = term if out is None else out + term
    return out.astype(jnp.bfloat16)


def project_home_kernel(attended_ref, weight_ref, out_ref):
    out_ref[...] = project(attended_ref, weight_ref, out_ref.shape[0], slice(None))


def finish_kernel(
    home_ref, other_ref, weight_ref, log_ref, out_hbm, log_hbm, out_ref, sems
):
    tok, width = out_ref.shape
    log_copy = pltpu.make_async_copy(log_ref, log_hbm, sems.at[0])
    log_copy.start()
    step = math.gcd(width, OUT_STEP)
    base = lax.axis_index("head") * width
    copies = [log_copy]
    for at in range(width // step):
        here = slice(at * step, (at + 1) * step)
        columns = pl.ds(pl.multiple_of(base + at * step, 128), step)
        other = project(other_ref, weight_ref, tok, columns)
        out_ref[:, here] = (
            home_ref[:, here].astype(jnp.float32) + other.astype(jnp.float32)
        ).astype(jnp.bfloat16)
        copies.append(
            pltpu.make_async_copy(
                out_ref.at[:, here], out_hbm.at[:, here], sems.at[1 + at]
            )
        )
        copies[-1].start()
    for copy in copies:
        copy.wait()


def cost(flops, moved, transcendentals=0):
    return pl.CostEstimate(flops=flops, bytes_accessed=moved, transcendentals=transcendentals)


def in_hbm(array):
    return pltpu.with_memory_space_constraint(array, pltpu.HBM)


def params(mib):
    return pltpu.CompilerParams(vmem_limit_bytes=mib * 2**20)


def body(queries, keys, values, stretch_order, out_weight):
    tok = queries.shape[0]
    kv_heads = keys.shape[1] // DH
    heads = kv_heads * GROUP
    width = out_weight.shape[1] // lax.axis_size("head")
    spans, span_len = lax.axis_size("blk"), lax.axis_size("rep")
    query, packed, bounds = pl.pallas_call(
        lambda *refs: pack_kernel(spans, span_len, *refs),
        out_shape=(
            jax.ShapeDtypeStruct((heads * tok, DH), jnp.bfloat16),
            jax.ShapeDtypeStruct((kv_heads, 2, tok, DH), jnp.bfloat16),
            jax.ShapeDtypeStruct((spans * span_len, tok), jnp.int32),
        ),
        in_specs=[HBM] * 4,
        out_specs=(VMEM, VMEM, VMEM),
        scratch_shapes=[
            pltpu.VMEM((tok, kv_heads * DH), jnp.bfloat16),
            pltpu.SMEM(stretch_order.shape, jnp.int32),
            pltpu.SemaphoreType.DMA((2 + kv_heads + heads,)),
        ],
        compiler_params=params(4),
        name="pack",
    )(*[in_hbm(x) for x in (queries, keys, values, stretch_order)])
    kv, query = [packed], [query]
    for hop in range(1, spans):
        kv.append(lax.ppermute(packed, "blk", hops_out(hop, spans)))
    for hop in range(1, span_len):
        query.append(lax.ppermute(query[0], "rep", hops_out(hop, span_len)))
    weight_away = lax.ppermute(out_weight, "head", [(0, 1), (1, 0)])
    part_shape = jax.ShapeDtypeStruct((DH + STAT_ROWS, heads * tok), jnp.bfloat16)
    attend = dict(
        cost_estimate=cost(
            4 * heads * tok * spans * tok * DH,
            2 * heads * tok * DH * 2 + spans * tok * DH * 4,
            heads * tok * spans * tok,
        ),
        compiler_params=params(16 if spans > 8 else 8),
    )
    chunks = heads * DH // math.gcd(heads * DH, 64)
    parts = [None]
    for hop in range(1, span_len):
        parts.append(
            pl.pallas_call(
                lambda *refs, hop=hop: attend_kernel(hop, spans, *refs),
                out_shape=part_shape,
                in_specs=[VMEM] * (2 + spans),
                out_specs=VMEM,
                name="attend",
                **attend,
            )(bounds, query[hop], *kv)
        )
    parts[0], weight = pl.pallas_call(
        lambda *refs: attend_fetch_kernel(spans, chunks, *refs),
        out_shape=(part_shape, jax.ShapeDtypeStruct((heads * DH, width), jnp.bfloat16)),
        in_specs=[VMEM] * (2 + spans) + [HBM],
        out_specs=(VMEM, VMEM),
        scratch_shapes=[pltpu.SemaphoreType.DMA((chunks,))],
        name="attend_fetch",
        **attend,
    )(bounds, query[0], *kv, in_hbm(out_weight))
    returned = [parts[0]]
    for hop in range(1, span_len):
        returned.append(lax.ppermute(parts[hop], "rep", hops_back(hop, span_len)))
    attended, log_sum = pl.pallas_call(
        combine_kernel,
        out_shape=(
            jax.ShapeDtypeStruct((DH, heads * tok), jnp.bfloat16),
            jax.ShapeDtypeStruct((heads, tok), jnp.float32),
        ),
        in_specs=[VMEM] * span_len,
        out_specs=(VMEM, VMEM),
        compiler_params=params(4),
        name="combine",
    )(*returned)
    other = lax.ppermute(attended, "head", [(0, 1), (1, 0)])
    shape = jax.ShapeDtypeStruct((tok, width), jnp.bfloat16)
    home = pl.pallas_call(
        project_home_kernel,
        out_shape=shape,
        in_specs=[VMEM, VMEM],
        out_specs=VMEM,
        cost_estimate=cost(2 * tok * heads * DH * width, heads * DH * width * 2),
        compiler_params=params(4),
        name="project_home",
    )(attended, weight)
    return pl.pallas_call(
        finish_kernel,
        out_shape=(shape, jax.ShapeDtypeStruct((heads, tok), jnp.float32)),
        in_specs=[VMEM, VMEM, VMEM, VMEM],
        out_specs=(HBM, HBM),
        scratch_shapes=[
            pltpu.VMEM((tok, width), jnp.bfloat16),
            pltpu.SemaphoreType.DMA((1 + width // math.gcd(width, OUT_STEP),)),
        ],
        compiler_params=params(4),
        name="finish",
    )(home, other, weight_away, log_sum)


def solution(mesh):
    in_specs = (
        P(("blk", "rep"), "head"),
        P(("blk", "rep"), "head"),
        P(("blk", "rep"), "head"),
        P(),
        P("head", None),
    )
    out_specs = (P(("blk", "rep"), "head"), P("head", ("blk", "rep")))

    return jax.shard_map(body, mesh=mesh, in_specs=in_specs, out_specs=out_specs, check_vma=False)
```

```python
import math

import jax
import jax.numpy as jnp
from jax import lax
from jax.experimental import pallas as pl
from jax.experimental.pallas import tpu as pltpu
from jax.sharding import PartitionSpec as P


GROUP = 3
DH = 128
NEG_FILL = -1e30
LOG2E = math.log2(math.e)
STAT_ROWS = 16
OUT_STEP = 512


VMEM = pl.BlockSpec(memory_space=pltpu.VMEM)
HBM = pl.BlockSpec(memory_space=pltpu.HBM)


def source_of(me, hop, count):
    if count & (count - 1) == 0:
        return lax.bitwise_xor(me, jnp.int32(hop))
    return lax.rem(me + (count - hop), count)


def hops_out(hop, count):
    if count & (count - 1) == 0:
        return [(i, i ^ hop) for i in range(count)]
    return [(i, (i + hop) % count) for i in range(count)]


def hops_back(hop, count):
    return [(b, a) for a, b in hops_out(hop, count)]


def pack_kernel(
    spans, span_len, query_hbm, keys_hbm, values_hbm, order_hbm,
    query_ref, packed_ref, bound_ref, values_ref, order_ref, sems,
):
    tok = values_ref.shape[0]
    heads, kv_heads = query_ref.shape[0] // tok, packed_ref.shape[0]
    order_copy = pltpu.make_async_copy(order_hbm, order_ref, sems.at[0])
    value_copy = pltpu.make_async_copy(values_hbm, values_ref, sems.at[1])
    copies = []
    for head in range(kv_heads):
        copies.append((keys_hbm.at[:, pl.ds(head * DH, DH)], packed_ref.at[head, 0]))
    for head in range(heads):
        copies.append(
            (query_hbm.at[:, pl.ds(head * DH, DH)], query_ref.at[pl.ds(head * tok, tok), :])
        )
    copies = [
        pltpu.make_async_copy(source, target, sems.at[2 + at])
        for at, (source, target) in enumerate(copies)
    ]
    value_copy.start()
    order_copy.start()
    for copy in copies:
        copy.start()
    value_copy.wait()
    for head in range(kv_heads):
        packed_ref[head, 1] = values_ref[:, head * DH : (head + 1) * DH].T
    order_copy.wait()
    blk_rank, rep_rank = lax.axis_index("blk"), lax.axis_index("rep")
    for rep_hop in range(span_len):
        query_at = blk_rank * span_len + source_of(rep_rank, rep_hop, span_len)
        for hop in range(spans):
            key_at = source_of(blk_rank, hop, spans) * span_len + rep_rank
            row = rep_hop * spans + hop
            bound_ref[row : row + 1, :] = jnp.full(
                (1, tok), (order_ref[query_at] - order_ref[key_at]) * tok, jnp.int32
            )
    for copy in copies:
        copy.wait()


def store_part(out_ref, kv_head, numer, top, total, factor):
    tok = out_ref.shape[1]
    heads = (out_ref.shape[0] - STAT_ROWS) // DH
    some = total > 0.0
    numer = (numer * jnp.where(some, 1.0 / total, 0.0)).astype(jnp.bfloat16)
    log_sum = top * factor + jnp.where(some, jnp.log(total), 0.0)
    high = log_sum.astype(jnp.bfloat16)
    rest = log_sum - high.astype(jnp.float32)
    middle = rest.astype(jnp.bfloat16)
    low = (rest - middle.astype(jnp.float32)).astype(jnp.bfloat16)
    for group in range(GROUP):
        head = kv_head * GROUP + group
        lanes = slice(group * tok, (group + 1) * tok)
        out_ref[head * DH : (head + 1) * DH, :] = numer[:, lanes]
        for at, stat in enumerate((high, middle, low)):
            row = heads * DH + 3 * head + at
            out_ref[row : row + 1, :] = stat[:, lanes]


def attend_kernel(rep_hop, spans, bound_ref, query_ref, *refs):
    kv_refs, out_ref = refs[:spans], refs[spans]
    tok = bound_ref.shape[1]
    kv_heads = kv_refs[0].shape[0]
    factor = DH**-0.5
    lanes = GROUP * tok
    for kv_head in range(kv_heads):
        query = query_ref[kv_head * lanes : (kv_head + 1) * lanes, :]
        scores, tops, allowed = [], [], []
        for hop in range(spans):
            raw = lax.dot_general(
                kv_refs[hop][kv_head, 0],
                query,
                (((1,), (1,)), ((), ())),
                preferred_element_type=jnp.float32,
            )
            at = rep_hop * spans + hop
            bound = jnp.concatenate([bound_ref[at : at + 1, :]] * GROUP, axis=1)
            if rep_hop == 0 and hop == 0:
                ahead = lax.broadcasted_iota(jnp.int32, (tok, tok), 0) - lax.broadcasted_iota(
                    jnp.int32, (tok, tok), 1
                )
                raw = jnp.where(jnp.concatenate([ahead] * GROUP, axis=1) <= 0, raw, NEG_FILL)
            scores.append(raw)
            allowed.append(bound >= 0)
            tops.append(
                jnp.where(bound >= 0, jnp.max(raw, axis=0, keepdims=True), NEG_FILL)
            )
        top = tops[0]
        for hop in range(1, spans):
            top = jnp.maximum(top, tops[hop])
        total, numer = None, None
        for hop in range(spans):
            chunk_top = jnp.where(allowed[hop], top, -NEG_FILL)
            weights = jnp.exp2((scores[hop] - chunk_top) * (factor * LOG2E))
            total = weights if total is None else total + weights
            term = lax.dot_general(
                kv_refs[hop][kv_head, 1],
                weights.astype(jnp.bfloat16),
                (((1,), (0,)), ((), ())),
                preferred_element_type=jnp.float32,
            )
            numer = term if numer is None else numer + term
        total = jnp.sum(total, axis=0, keepdims=True)
        store_part(out_ref, kv_head, numer, top, total, factor)


def attend_fetch_kernel(spans, chunks, *refs):
    weight_hbm, part_ref, weight_ref, sems = refs[-4:]
    rows, width = weight_ref.shape[0] // chunks, weight_ref.shape[1]
    columns = pl.ds(pl.multiple_of(lax.axis_index("head") * width, 128), width)
    copies = []
    for chunk in range(chunks):
        here = pl.ds(chunk * rows, rows)
        copies.append(
            pltpu.make_async_copy(
                weight_hbm.at[here, columns], weight_ref.at[here, :], sems.at[chunk]
            )
        )
        copies[-1].start()
    attend_kernel(0, spans, *refs[:-4], part_ref)
    for copy in copies:
        copy.wait()


def combine_kernel(*refs):
    part_refs, (attended_ref, log_sum_ref) = refs[:-2], refs[-2:]
    heads, _ = log_sum_ref.shape
    for head in range(heads):
        stats = []
        for part in part_refs:
            parts = part[heads * DH : heads * DH + STAT_ROWS, :].astype(jnp.float32)
            row = 3 * head
            stats.append(parts[row : row + 1] + parts[row + 1 : row + 2] + parts[row + 2 : row + 3])
        top = stats[0]
        for stat in stats[1:]:
            top = jnp.maximum(top, stat)
        shares = [jnp.exp(stat - top) for stat in stats]
        total = shares[0]
        for share in shares[1:]:
            total = total + share
        scale = 1.0 / total
        rows = slice(head * DH, (head + 1) * DH)
        numer = None
        for part, share in zip(part_refs, shares):
            term = part[rows, :].astype(jnp.float32) * (share * scale)
            numer = term if numer is None else numer + term
        attended_ref[rows, :] = numer.astype(jnp.bfloat16)
        log_sum_ref[head : head + 1, :] = top + jnp.log(total)


def project(attended_ref, weight_ref, columns):
    out = None
    for head in range(weight_ref.shape[0] // DH):
        term = lax.dot_general(
            attended_ref[head * DH : (head + 1) * DH, :],
            weight_ref[head * DH : (head + 1) * DH, columns],
            (((0,), (0,)), ((), ())),
            preferred_element_type=jnp.float32,
        )
        out = term if out is None else out + term
    return out.astype(jnp.bfloat16)


def project_home_kernel(attended_ref, weight_ref, out_ref):
    out_ref[...] = project(attended_ref, weight_ref, slice(None))


def finish_kernel(
    home_ref, other_ref, weight_ref, log_ref, out_hbm, log_hbm, out_ref, sems
):
    width = out_ref.shape[1]
    log_copy = pltpu.make_async_copy(log_ref, log_hbm, sems.at[0])
    log_copy.start()
    step = math.gcd(width, OUT_STEP)
    base = lax.axis_index("head") * width
    copies = [log_copy]
    for at in range(width // step):
        here = slice(at * step, (at + 1) * step)
        columns = pl.ds(pl.multiple_of(base + at * step, 128), step)
        other = project(other_ref, weight_ref, columns)
        out_ref[:, here] = (
            home_ref[:, here].astype(jnp.float32) + other.astype(jnp.float32)
        ).astype(jnp.bfloat16)
        copies.append(
            pltpu.make_async_copy(
                out_ref.at[:, here], out_hbm.at[:, here], sems.at[1 + at]
            )
        )
        copies[-1].start()
    for copy in copies:
        copy.wait()


def cost(flops, moved, transcendentals=0):
    return pl.CostEstimate(flops=flops, bytes_accessed=moved, transcendentals=transcendentals)


def in_hbm(array):
    return pltpu.with_memory_space_constraint(array, pltpu.HBM)


def params(mib):
    return pltpu.CompilerParams(vmem_limit_bytes=mib * 2**20)


def body(queries, keys, values, stretch_order, out_weight):
    tok = queries.shape[0]
    kv_heads = keys.shape[1] // DH
    heads = kv_heads * GROUP
    width = out_weight.shape[1] // lax.axis_size("head")
    spans, span_len = lax.axis_size("blk"), lax.axis_size("rep")
    query, packed, bounds = pl.pallas_call(
        lambda *refs: pack_kernel(spans, span_len, *refs),
        out_shape=(
            jax.ShapeDtypeStruct((heads * tok, DH), jnp.bfloat16),
            jax.ShapeDtypeStruct((kv_heads, 2, tok, DH), jnp.bfloat16),
            jax.ShapeDtypeStruct((spans * span_len, tok), jnp.int32),
        ),
        in_specs=[HBM] * 4,
        out_specs=(VMEM, VMEM, VMEM),
        scratch_shapes=[
            pltpu.VMEM((tok, kv_heads * DH), jnp.bfloat16),
            pltpu.SMEM(stretch_order.shape, jnp.int32),
            pltpu.SemaphoreType.DMA((2 + kv_heads + heads,)),
        ],
        compiler_params=params(4),
        name="pack",
    )(*[in_hbm(x) for x in (queries, keys, values, stretch_order)])
    kv, query = [packed], [query]
    for hop in range(1, spans):
        kv.append(lax.ppermute(packed, "blk", hops_out(hop, spans)))
    for hop in range(1, span_len):
        query.append(lax.ppermute(query[0], "rep", hops_out(hop, span_len)))
    weight_away = lax.ppermute(out_weight, "head", [(0, 1), (1, 0)])
    part_shape = jax.ShapeDtypeStruct((heads * DH + STAT_ROWS, tok), jnp.bfloat16)
    attend = dict(
        cost_estimate=cost(
            4 * heads * tok * spans * tok * DH,
            2 * heads * tok * DH * 2 + spans * tok * DH * 4,
            heads * tok * spans * tok,
        ),
        compiler_params=params(16 if spans > 8 else 8),
    )
    chunks = heads * DH // math.gcd(heads * DH, 64)
    parts = [None]
    for hop in range(1, span_len):
        parts.append(
            pl.pallas_call(
                lambda *refs, hop=hop: attend_kernel(hop, spans, *refs),
                out_shape=part_shape,
                in_specs=[VMEM] * (2 + spans),
                out_specs=VMEM,
                name="attend",
                **attend,
            )(bounds, query[hop], *kv)
        )
    parts[0], weight = pl.pallas_call(
        lambda *refs: attend_fetch_kernel(spans, chunks, *refs),
        out_shape=(part_shape, jax.ShapeDtypeStruct((heads * DH, width), jnp.bfloat16)),
        in_specs=[VMEM] * (2 + spans) + [HBM],
        out_specs=(VMEM, VMEM),
        scratch_shapes=[pltpu.SemaphoreType.DMA((chunks,))],
        name="attend_fetch",
        **attend,
    )(bounds, query[0], *kv, in_hbm(out_weight))
    returned = [parts[0]]
    for hop in range(1, span_len):
        returned.append(lax.ppermute(parts[hop], "rep", hops_back(hop, span_len)))
    attended, log_sum = pl.pallas_call(
        combine_kernel,
        out_shape=(
            jax.ShapeDtypeStruct((heads * DH, tok), jnp.bfloat16),
            jax.ShapeDtypeStruct((heads, tok), jnp.float32),
        ),
        in_specs=[VMEM] * span_len,
        out_specs=(VMEM, VMEM),
        compiler_params=params(4),
        name="combine",
    )(*returned)
    other = lax.ppermute(attended, "head", [(0, 1), (1, 0)])
    shape = jax.ShapeDtypeStruct((tok, width), jnp.bfloat16)
    home = pl.pallas_call(
        project_home_kernel,
        out_shape=shape,
        in_specs=[VMEM, VMEM],
        out_specs=VMEM,
        cost_estimate=cost(2 * tok * heads * DH * width, heads * DH * width * 2),
        compiler_params=params(4),
        name="project_home",
    )(attended, weight)
    return pl.pallas_call(
        finish_kernel,
        out_shape=(shape, jax.ShapeDtypeStruct((heads, tok), jnp.float32)),
        in_specs=[VMEM, VMEM, VMEM, VMEM],
        out_specs=(HBM, HBM),
        scratch_shapes=[
            pltpu.VMEM((tok, width), jnp.bfloat16),
            pltpu.SemaphoreType.DMA((1 + width // math.gcd(width, OUT_STEP),)),
        ],
        compiler_params=params(4),
        name="finish",
    )(home, other, weight_away, log_sum)


def solution(mesh):
    in_specs = (
        P(("blk", "rep"), "head"),
        P(("blk", "rep"), "head"),
        P(("blk", "rep"), "head"),
        P(),
        P("head", None),
    )
    out_specs = (P(("blk", "rep"), "head"), P("head", ("blk", "rep")))

    return jax.shard_map(body, mesh=mesh, in_specs=in_specs, out_specs=out_specs, check_vma=False)
```

```python
import math

import jax
import jax.numpy as jnp
from jax import lax
from jax.experimental import pallas as pl
from jax.experimental.pallas import tpu as pltpu
from jax.sharding import PartitionSpec as P


GROUP = 3
DH = 128
NEG_FILL = -1e30
LOG2E = math.log2(math.e)
STAT_ROWS = 16
OUT_STEP = 512


VMEM = pl.BlockSpec(memory_space=pltpu.VMEM)
HBM = pl.BlockSpec(memory_space=pltpu.HBM)


def source_of(me, hop, count):
    if count & (count - 1) == 0:
        return lax.bitwise_xor(me, jnp.int32(hop))
    return lax.rem(me + (count - hop), count)


def hops_out(hop, count):
    if count & (count - 1) == 0:
        return [(i, i ^ hop) for i in range(count)]
    return [(i, (i + hop) % count) for i in range(count)]


def hops_back(hop, count):
    return [(b, a) for a, b in hops_out(hop, count)]


def pack_kernel(
    spans, span_len, query_hbm, keys_hbm, values_hbm, order_hbm,
    query_ref, packed_ref, bound_ref, values_ref, order_ref, sems,
):
    tok = values_ref.shape[0]
    heads, kv_heads = query_ref.shape[0] // tok, packed_ref.shape[0]
    order_copy = pltpu.make_async_copy(order_hbm, order_ref, sems.at[0])
    value_copy = pltpu.make_async_copy(values_hbm, values_ref, sems.at[1])
    copies = []
    for head in range(kv_heads):
        copies.append((keys_hbm.at[:, pl.ds(head * DH, DH)], packed_ref.at[head, 0]))
    for head in range(heads):
        copies.append(
            (query_hbm.at[:, pl.ds(head * DH, DH)], query_ref.at[pl.ds(head * tok, tok), :])
        )
    copies = [
        pltpu.make_async_copy(source, target, sems.at[2 + at])
        for at, (source, target) in enumerate(copies)
    ]
    value_copy.start()
    order_copy.start()
    for copy in copies:
        copy.start()
    value_copy.wait()
    for head in range(kv_heads):
        packed_ref[head, 1] = values_ref[:, head * DH : (head + 1) * DH].T
    order_copy.wait()
    blk_rank, rep_rank = lax.axis_index("blk"), lax.axis_index("rep")
    for rep_hop in range(span_len):
        query_at = blk_rank * span_len + source_of(rep_rank, rep_hop, span_len)
        for hop in range(spans):
            key_at = source_of(blk_rank, hop, spans) * span_len + rep_rank
            row = rep_hop * spans + hop
            bound_ref[row : row + 1, :] = jnp.full(
                (1, tok), (order_ref[query_at] - order_ref[key_at]) * tok, jnp.int32
            )
    for copy in copies:
        copy.wait()


def store_part(out_ref, kv_head, numer, top, total, factor):
    tok = out_ref.shape[1]
    heads = (out_ref.shape[0] - STAT_ROWS) // DH
    some = total > 0.0
    numer = (numer * jnp.where(some, 1.0 / total, 0.0)).astype(jnp.bfloat16)
    log_sum = top * factor + jnp.where(some, jnp.log(total), 0.0)
    high = log_sum.astype(jnp.bfloat16)
    rest = log_sum - high.astype(jnp.float32)
    middle = rest.astype(jnp.bfloat16)
    low = (rest - middle.astype(jnp.float32)).astype(jnp.bfloat16)
    for group in range(GROUP):
        head = kv_head * GROUP + group
        lanes = slice(group * tok, (group + 1) * tok)
        out_ref[head * DH : (head + 1) * DH, :] = numer[:, lanes]
        for at, stat in enumerate((high, middle, low)):
            row = heads * DH + 3 * head + at
            out_ref[row : row + 1, :] = stat[:, lanes]


def attend_kernel(rep_hop, spans, bound_ref, query_ref, *refs):
    kv_refs, out_ref = refs[:spans], refs[spans]
    tok = bound_ref.shape[1]
    kv_heads = kv_refs[0].shape[0]
    factor = DH**-0.5
    lanes = GROUP * tok
    for kv_head in range(kv_heads):
        query = query_ref[kv_head * lanes : (kv_head + 1) * lanes, :]
        scores, allowed, top = [], [], None
        for first in range(0, spans, 2):
            pair = kv_refs[first : first + 2]
            raw = lax.dot_general(
                jnp.concatenate([ref[kv_head, 0] for ref in pair], axis=0),
                query,
                (((1,), (1,)), ((), ())),
                preferred_element_type=jnp.float32,
            )
            for at in range(len(pair)):
                hop = first + at
                chunk = raw[at * tok : (at + 1) * tok, :]
                if rep_hop == 0 and hop == 0:
                    ahead = lax.broadcasted_iota(jnp.int32, (tok, tok), 0)
                    ahead = ahead - lax.broadcasted_iota(jnp.int32, (tok, tok), 1)
                    ahead = jnp.concatenate([ahead] * GROUP, axis=1)
                    chunk = jnp.where(ahead <= 0, chunk, NEG_FILL)
                row = rep_hop * spans + hop
                bound = jnp.concatenate([bound_ref[row : row + 1, :]] * GROUP, axis=1)
                scores.append(chunk)
                allowed.append(bound >= 0)
                chunk_top = jnp.max(chunk, axis=0, keepdims=True)
                chunk_top = jnp.where(allowed[hop], chunk_top, NEG_FILL)
                top = chunk_top if top is None else jnp.maximum(top, chunk_top)
        total, numer = None, None
        for first in range(0, spans, 2):
            pair, weights = kv_refs[first : first + 2], []
            for hop in range(first, first + len(pair)):
                chunk_top = jnp.where(allowed[hop], top, -NEG_FILL)
                weight = jnp.exp2((scores[hop] - chunk_top) * (factor * LOG2E))
                total = weight if total is None else total + weight
                weights.append(weight.astype(jnp.bfloat16))
            term = lax.dot_general(
                jnp.concatenate([ref[kv_head, 1] for ref in pair], axis=1),
                jnp.concatenate(weights, axis=0),
                (((1,), (0,)), ((), ())),
                preferred_element_type=jnp.float32,
            )
            numer = term if numer is None else numer + term
        total = jnp.sum(total, axis=0, keepdims=True)
        store_part(out_ref, kv_head, numer, top, total, factor)


def attend_fetch_kernel(spans, chunks, *refs):
    weight_hbm, part_ref, weight_ref, sems = refs[-4:]
    rows, width = weight_ref.shape[0] // chunks, weight_ref.shape[1]
    columns = pl.ds(pl.multiple_of(lax.axis_index("head") * width, 128), width)
    copies = []
    for chunk in range(chunks):
        here = pl.ds(chunk * rows, rows)
        copies.append(
            pltpu.make_async_copy(
                weight_hbm.at[here, columns], weight_ref.at[here, :], sems.at[chunk]
            )
        )
        copies[-1].start()
    attend_kernel(0, spans, *refs[:-4], part_ref)
    for copy in copies:
        copy.wait()


def combine_kernel(*refs):
    part_refs, (attended_ref, log_sum_ref) = refs[:-2], refs[-2:]
    heads, _ = log_sum_ref.shape
    for head in range(heads):
        stats = []
        for part in part_refs:
            parts = part[heads * DH : heads * DH + STAT_ROWS, :].astype(jnp.float32)
            row = 3 * head
            stats.append(parts[row : row + 1] + parts[row + 1 : row + 2] + parts[row + 2 : row + 3])
        top = stats[0]
        for stat in stats[1:]:
            top = jnp.maximum(top, stat)
        shares = [jnp.exp(stat - top) for stat in stats]
        total = shares[0]
        for share in shares[1:]:
            total = total + share
        scale = 1.0 / total
        rows = slice(head * DH, (head + 1) * DH)
        numer = None
        for part, share in zip(part_refs, shares):
            term = part[rows, :].astype(jnp.float32) * (share * scale)
            numer = term if numer is None else numer + term
        attended_ref[rows, :] = numer.astype(jnp.bfloat16)
        log_sum_ref[head : head + 1, :] = top + jnp.log(total)


def project(attended_ref, weight_ref, columns):
    return lax.dot_general(
        attended_ref[...],
        weight_ref[:, columns],
        (((0,), (0,)), ((), ())),
        preferred_element_type=jnp.float32,
    ).astype(jnp.bfloat16)


def project_home_kernel(attended_ref, weight_ref, out_ref):
    out_ref[...] = project(attended_ref, weight_ref, slice(None))


def finish_kernel(
    home_ref, other_ref, weight_ref, log_ref, out_hbm, log_hbm, out_ref, sems
):
    width = out_ref.shape[1]
    log_copy = pltpu.make_async_copy(log_ref, log_hbm, sems.at[0])
    log_copy.start()
    step = math.gcd(width, OUT_STEP)
    base = lax.axis_index("head") * width
    copies = [log_copy]
    for at in range(width // step):
        here = slice(at * step, (at + 1) * step)
        columns = pl.ds(pl.multiple_of(base + at * step, 128), step)
        other = project(other_ref, weight_ref, columns)
        out_ref[:, here] = (
            home_ref[:, here].astype(jnp.float32) + other.astype(jnp.float32)
        ).astype(jnp.bfloat16)
        copies.append(
            pltpu.make_async_copy(
                out_ref.at[:, here], out_hbm.at[:, here], sems.at[1 + at]
            )
        )
        copies[-1].start()
    for copy in copies:
        copy.wait()


def cost(flops, moved, transcendentals=0):
    return pl.CostEstimate(flops=flops, bytes_accessed=moved, transcendentals=transcendentals)


def in_hbm(array):
    return pltpu.with_memory_space_constraint(array, pltpu.HBM)


def params(mib):
    return pltpu.CompilerParams(vmem_limit_bytes=mib * 2**20)


def body(queries, keys, values, stretch_order, out_weight):
    tok = queries.shape[0]
    kv_heads = keys.shape[1] // DH
    heads = kv_heads * GROUP
    width = out_weight.shape[1] // lax.axis_size("head")
    spans, span_len = lax.axis_size("blk"), lax.axis_size("rep")
    query, packed, bounds = pl.pallas_call(
        lambda *refs: pack_kernel(spans, span_len, *refs),
        out_shape=(
            jax.ShapeDtypeStruct((heads * tok, DH), jnp.bfloat16),
            jax.ShapeDtypeStruct((kv_heads, 2, tok, DH), jnp.bfloat16),
            jax.ShapeDtypeStruct((spans * span_len, tok), jnp.int32),
        ),
        in_specs=[HBM] * 4,
        out_specs=(VMEM, VMEM, VMEM),
        scratch_shapes=[
            pltpu.VMEM((tok, kv_heads * DH), jnp.bfloat16),
            pltpu.SMEM(stretch_order.shape, jnp.int32),
            pltpu.SemaphoreType.DMA((2 + kv_heads + heads,)),
        ],
        compiler_params=params(4),
        name="pack",
    )(*[in_hbm(x) for x in (queries, keys, values, stretch_order)])
    kv, query = [packed], [query]
    for hop in range(1, spans):
        kv.append(lax.ppermute(packed, "blk", hops_out(hop, spans)))
    for hop in range(1, span_len):
        query.append(lax.ppermute(query[0], "rep", hops_out(hop, span_len)))
    weight_away = lax.ppermute(out_weight, "head", [(0, 1), (1, 0)])
    part_shape = jax.ShapeDtypeStruct((heads * DH + STAT_ROWS, tok), jnp.bfloat16)
    attend = dict(
        cost_estimate=cost(
            4 * heads * tok * spans * tok * DH,
            2 * heads * tok * DH * 2 + spans * tok * DH * 4,
            heads * tok * spans * tok,
        ),
        compiler_params=params(16 if spans > 8 else 8),
    )
    chunks = heads * DH // math.gcd(heads * DH, 64)
    parts = [None]
    for hop in range(1, span_len):
        parts.append(
            pl.pallas_call(
                lambda *refs, hop=hop: attend_kernel(hop, spans, *refs),
                out_shape=part_shape,
                in_specs=[VMEM] * (2 + spans),
                out_specs=VMEM,
                name="attend",
                **attend,
            )(bounds, query[hop], *kv)
        )
    parts[0], weight = pl.pallas_call(
        lambda *refs: attend_fetch_kernel(spans, chunks, *refs),
        out_shape=(part_shape, jax.ShapeDtypeStruct((heads * DH, width), jnp.bfloat16)),
        in_specs=[VMEM] * (2 + spans) + [HBM],
        out_specs=(VMEM, VMEM),
        scratch_shapes=[pltpu.SemaphoreType.DMA((chunks,))],
        name="attend_fetch",
        **attend,
    )(bounds, query[0], *kv, in_hbm(out_weight))
    returned = [parts[0]]
    for hop in range(1, span_len):
        returned.append(lax.ppermute(parts[hop], "rep", hops_back(hop, span_len)))
    attended, log_sum = pl.pallas_call(
        combine_kernel,
        out_shape=(
            jax.ShapeDtypeStruct((heads * DH, tok), jnp.bfloat16),
            jax.ShapeDtypeStruct((heads, tok), jnp.float32),
        ),
        in_specs=[VMEM] * span_len,
        out_specs=(VMEM, VMEM),
        compiler_params=params(4),
        name="combine",
    )(*returned)
    other = lax.ppermute(attended, "head", [(0, 1), (1, 0)])
    shape = jax.ShapeDtypeStruct((tok, width), jnp.bfloat16)
    home = pl.pallas_call(
        project_home_kernel,
        out_shape=shape,
        in_specs=[VMEM, VMEM],
        out_specs=VMEM,
        cost_estimate=cost(2 * tok * heads * DH * width, heads * DH * width * 2),
        compiler_params=params(4),
        name="project_home",
    )(attended, weight)
    return pl.pallas_call(
        finish_kernel,
        out_shape=(shape, jax.ShapeDtypeStruct((heads, tok), jnp.float32)),
        in_specs=[VMEM, VMEM, VMEM, VMEM],
        out_specs=(HBM, HBM),
        scratch_shapes=[
            pltpu.VMEM((tok, width), jnp.bfloat16),
            pltpu.SemaphoreType.DMA((1 + width // math.gcd(width, OUT_STEP),)),
        ],
        compiler_params=params(4),
        name="finish",
    )(home, other, weight_away, log_sum)


def solution(mesh):
    in_specs = (
        P(("blk", "rep"), "head"),
        P(("blk", "rep"), "head"),
        P(("blk", "rep"), "head"),
        P(),
        P("head", None),
    )
    out_specs = (P(("blk", "rep"), "head"), P("head", ("blk", "rep")))

    return jax.shard_map(body, mesh=mesh, in_specs=in_specs, out_specs=out_specs, check_vma=False)
```

```python
import math

import jax
import jax.numpy as jnp
from jax import lax
from jax.experimental import pallas as pl
from jax.experimental.pallas import tpu as pltpu
from jax.sharding import PartitionSpec as P


GROUP = 3
DH = 128
NEG_FILL = -1e30
LOG2E = math.log2(math.e)
STAT_ROWS = 16
OUT_STEP = 512


VMEM = pl.BlockSpec(memory_space=pltpu.VMEM)
HBM = pl.BlockSpec(memory_space=pltpu.HBM)


def source_of(me, hop, count):
    if count & (count - 1) == 0:
        return lax.bitwise_xor(me, jnp.int32(hop))
    return lax.rem(me + (count - hop), count)


def hops_out(hop, count):
    if count & (count - 1) == 0:
        return [(i, i ^ hop) for i in range(count)]
    return [(i, (i + hop) % count) for i in range(count)]


def hops_back(hop, count):
    return [(b, a) for a, b in hops_out(hop, count)]


def pack_kernel(
    spans, span_len, query_hbm, keys_hbm, values_hbm, order_hbm,
    query_ref, packed_ref, bound_ref, order_ref, sems,
):
    kv_heads, _, tok, _ = packed_ref.shape
    heads = query_ref.shape[0] // tok
    order_copy = pltpu.make_async_copy(order_hbm, order_ref, sems.at[0])
    copies = []
    for head in range(kv_heads):
        columns = pl.ds(head * DH, DH)
        copies.append((keys_hbm.at[:, columns], packed_ref.at[head, 0]))
        copies.append((values_hbm.at[:, columns], packed_ref.at[head, 1]))
    for head in range(heads):
        copies.append(
            (query_hbm.at[:, pl.ds(head * DH, DH)], query_ref.at[pl.ds(head * tok, tok), :])
        )
    copies = [
        pltpu.make_async_copy(source, target, sems.at[1 + at])
        for at, (source, target) in enumerate(copies)
    ]
    order_copy.start()
    for copy in copies:
        copy.start()
    order_copy.wait()
    blk_rank, rep_rank = lax.axis_index("blk"), lax.axis_index("rep")
    for rep_hop in range(span_len):
        query_at = blk_rank * span_len + source_of(rep_rank, rep_hop, span_len)
        for hop in range(spans):
            key_at = source_of(blk_rank, hop, spans) * span_len + rep_rank
            row = rep_hop * spans + hop
            bound_ref[row : row + 1, :] = jnp.full(
                (1, tok), (order_ref[query_at] - order_ref[key_at]) * tok, jnp.int32
            )
    for copy in copies:
        copy.wait()


def prepare_kernel(*refs):
    kv_refs, (keys_ref, values_ref) = refs[:-2], refs[-2:]
    for at, ref in enumerate(kv_refs):
        kv_heads, _, tok, _ = ref.shape
        here = slice(at * tok, (at + 1) * tok)
        for kv_head in range(kv_heads):
            keys_ref[kv_head, here, :] = ref[kv_head, 0]
            values_ref[kv_head, :, here] = ref[kv_head, 1].T


def store_part(out_ref, kv_head, numer, top, total, factor):
    tok = out_ref.shape[1]
    heads = (out_ref.shape[0] - STAT_ROWS) // DH
    some = total > 0.0
    numer = (numer * jnp.where(some, 1.0 / total, 0.0)).astype(jnp.bfloat16)
    log_sum = top * factor + jnp.where(some, jnp.log(total), 0.0)
    high = log_sum.astype(jnp.bfloat16)
    rest = log_sum - high.astype(jnp.float32)
    middle = rest.astype(jnp.bfloat16)
    low = (rest - middle.astype(jnp.float32)).astype(jnp.bfloat16)
    for group in range(GROUP):
        head = kv_head * GROUP + group
        lanes = slice(group * tok, (group + 1) * tok)
        out_ref[head * DH : (head + 1) * DH, :] = numer[:, lanes]
        for at, stat in enumerate((high, middle, low)):
            row = heads * DH + 3 * head + at
            out_ref[row : row + 1, :] = stat[:, lanes]


def attend_kernel(rep_hop, spans, bound_ref, query_ref, keys_ref, values_ref, out_ref):
    tok = bound_ref.shape[1]
    kv_heads = keys_ref.shape[0]
    factor = DH**-0.5
    lanes = GROUP * tok
    for kv_head in range(kv_heads):
        query = query_ref[kv_head * lanes : (kv_head + 1) * lanes, :]
        scores, allowed, top = [], [], None
        for first in range(0, spans, 2):
            count = min(2, spans - first)
            raw = lax.dot_general(
                keys_ref[kv_head, first * tok : (first + count) * tok, :],
                query,
                (((1,), (1,)), ((), ())),
                preferred_element_type=jnp.float32,
            )
            for at in range(count):
                hop = first + at
                chunk = raw[at * tok : (at + 1) * tok, :]
                if rep_hop == 0 and hop == 0:
                    ahead = lax.broadcasted_iota(jnp.int32, (tok, tok), 0)
                    ahead = ahead - lax.broadcasted_iota(jnp.int32, (tok, tok), 1)
                    ahead = jnp.concatenate([ahead] * GROUP, axis=1)
                    chunk = jnp.where(ahead <= 0, chunk, NEG_FILL)
                row = rep_hop * spans + hop
                bound = jnp.concatenate([bound_ref[row : row + 1, :]] * GROUP, axis=1)
                scores.append(chunk)
                allowed.append(bound >= 0)
                chunk_top = jnp.max(chunk, axis=0, keepdims=True)
                chunk_top = jnp.where(allowed[hop], chunk_top, NEG_FILL)
                top = chunk_top if top is None else jnp.maximum(top, chunk_top)
        total, numer = None, None
        for first in range(0, spans, 2):
            count, weights = min(2, spans - first), []
            for hop in range(first, first + count):
                chunk_top = jnp.where(allowed[hop], top, -NEG_FILL)
                weight = jnp.exp2((scores[hop] - chunk_top) * (factor * LOG2E))
                total = weight if total is None else total + weight
                weights.append(weight.astype(jnp.bfloat16))
            term = lax.dot_general(
                values_ref[kv_head, :, first * tok : (first + count) * tok],
                jnp.concatenate(weights, axis=0),
                (((1,), (0,)), ((), ())),
                preferred_element_type=jnp.float32,
            )
            numer = term if numer is None else numer + term
        total = jnp.sum(total, axis=0, keepdims=True)
        store_part(out_ref, kv_head, numer, top, total, factor)


def attend_fetch_kernel(spans, chunks, *refs):
    weight_hbm, part_ref, weight_ref, sems = refs[-4:]
    rows, width = weight_ref.shape[0] // chunks, weight_ref.shape[1]
    columns = pl.ds(pl.multiple_of(lax.axis_index("head") * width, 128), width)
    copies = []
    for chunk in range(chunks):
        here = pl.ds(chunk * rows, rows)
        copies.append(
            pltpu.make_async_copy(
                weight_hbm.at[here, columns], weight_ref.at[here, :], sems.at[chunk]
            )
        )
        copies[-1].start()
    attend_kernel(0, spans, *refs[:-4], part_ref)
    for copy in copies:
        copy.wait()


def combine_kernel(*refs):
    part_refs, (attended_ref, log_sum_ref) = refs[:-2], refs[-2:]
    heads, _ = log_sum_ref.shape
    for head in range(heads):
        stats = []
        for part in part_refs:
            parts = part[heads * DH : heads * DH + STAT_ROWS, :].astype(jnp.float32)
            row = 3 * head
            stats.append(parts[row : row + 1] + parts[row + 1 : row + 2] + parts[row + 2 : row + 3])
        top = stats[0]
        for stat in stats[1:]:
            top = jnp.maximum(top, stat)
        shares = [jnp.exp(stat - top) for stat in stats]
        total = shares[0]
        for share in shares[1:]:
            total = total + share
        scale = 1.0 / total
        rows = slice(head * DH, (head + 1) * DH)
        numer = None
        for part, share in zip(part_refs, shares):
            term = part[rows, :].astype(jnp.float32) * (share * scale)
            numer = term if numer is None else numer + term
        attended_ref[rows, :] = numer.astype(jnp.bfloat16)
        log_sum_ref[head : head + 1, :] = top + jnp.log(total)


def project(attended_ref, weight_ref, columns):
    return lax.dot_general(
        attended_ref[...],
        weight_ref[:, columns],
        (((0,), (0,)), ((), ())),
        preferred_element_type=jnp.float32,
    ).astype(jnp.bfloat16)


def project_home_kernel(attended_ref, weight_ref, out_ref):
    out_ref[...] = project(attended_ref, weight_ref, slice(None))


def finish_kernel(
    home_ref, other_ref, weight_ref, log_ref, out_hbm, log_hbm, out_ref, sems
):
    width = out_ref.shape[1]
    log_copy = pltpu.make_async_copy(log_ref, log_hbm, sems.at[0])
    log_copy.start()
    step = math.gcd(width, OUT_STEP)
    base = lax.axis_index("head") * width
    copies = [log_copy]
    for at in range(width // step):
        here = slice(at * step, (at + 1) * step)
        columns = pl.ds(pl.multiple_of(base + at * step, 128), step)
        other = project(other_ref, weight_ref, columns)
        out_ref[:, here] = (
            home_ref[:, here].astype(jnp.float32) + other.astype(jnp.float32)
        ).astype(jnp.bfloat16)
        copies.append(
            pltpu.make_async_copy(
                out_ref.at[:, here], out_hbm.at[:, here], sems.at[1 + at]
            )
        )
        copies[-1].start()
    for copy in copies:
        copy.wait()


def cost(flops, moved, transcendentals=0):
    return pl.CostEstimate(flops=flops, bytes_accessed=moved, transcendentals=transcendentals)


def in_hbm(array):
    return pltpu.with_memory_space_constraint(array, pltpu.HBM)


def params(mib):
    return pltpu.CompilerParams(vmem_limit_bytes=mib * 2**20)


def body(queries, keys, values, stretch_order, out_weight):
    tok = queries.shape[0]
    kv_heads = keys.shape[1] // DH
    heads = kv_heads * GROUP
    width = out_weight.shape[1] // lax.axis_size("head")
    spans, span_len = lax.axis_size("blk"), lax.axis_size("rep")
    query, packed, bounds = pl.pallas_call(
        lambda *refs: pack_kernel(spans, span_len, *refs),
        out_shape=(
            jax.ShapeDtypeStruct((heads * tok, DH), jnp.bfloat16),
            jax.ShapeDtypeStruct((kv_heads, 2, tok, DH), jnp.bfloat16),
            jax.ShapeDtypeStruct((spans * span_len, tok), jnp.int32),
        ),
        in_specs=[HBM] * 4,
        out_specs=(VMEM, VMEM, VMEM),
        scratch_shapes=[
            pltpu.SMEM(stretch_order.shape, jnp.int32),
            pltpu.SemaphoreType.DMA((1 + 2 * kv_heads + heads,)),
        ],
        compiler_params=params(4),
        name="pack",
    )(*[in_hbm(x) for x in (queries, keys, values, stretch_order)])
    kv, query = [packed], [query]
    for hop in range(1, spans):
        kv.append(lax.ppermute(packed, "blk", hops_out(hop, spans)))
    for hop in range(1, span_len):
        query.append(lax.ppermute(query[0], "rep", hops_out(hop, span_len)))
    weight_away = lax.ppermute(out_weight, "head", [(0, 1), (1, 0)])
    keys_all, values_all = pl.pallas_call(
        prepare_kernel,
        out_shape=(
            jax.ShapeDtypeStruct((kv_heads, spans * tok, DH), jnp.bfloat16),
            jax.ShapeDtypeStruct((kv_heads, DH, spans * tok), jnp.bfloat16),
        ),
        in_specs=[VMEM] * spans,
        out_specs=(VMEM, VMEM),
        compiler_params=params(8),
        name="prepare",
    )(*kv)
    part_shape = jax.ShapeDtypeStruct((heads * DH + STAT_ROWS, tok), jnp.bfloat16)
    attend = dict(
        cost_estimate=cost(
            4 * heads * tok * spans * tok * DH,
            2 * heads * tok * DH * 2 + spans * tok * DH * 4,
            heads * tok * spans * tok,
        ),
        compiler_params=params(16 if spans > 8 else 8),
    )
    chunks = heads * DH // math.gcd(heads * DH, 64)
    parts = [None]
    for hop in range(1, span_len):
        parts.append(
            pl.pallas_call(
                lambda *refs, hop=hop: attend_kernel(hop, spans, *refs),
                out_shape=part_shape,
                in_specs=[VMEM] * 4,
                out_specs=VMEM,
                name="attend",
                **attend,
            )(bounds, query[hop], keys_all, values_all)
        )
    parts[0], weight = pl.pallas_call(
        lambda *refs: attend_fetch_kernel(spans, chunks, *refs),
        out_shape=(part_shape, jax.ShapeDtypeStruct((heads * DH, width), jnp.bfloat16)),
        in_specs=[VMEM] * 4 + [HBM],
        out_specs=(VMEM, VMEM),
        scratch_shapes=[pltpu.SemaphoreType.DMA((chunks,))],
        name="attend_fetch",
        **attend,
    )(bounds, query[0], keys_all, values_all, in_hbm(out_weight))
    returned = [parts[0]]
    for hop in range(1, span_len):
        returned.append(lax.ppermute(parts[hop], "rep", hops_back(hop, span_len)))
    attended, log_sum = pl.pallas_call(
        combine_kernel,
        out_shape=(
            jax.ShapeDtypeStruct((heads * DH, tok), jnp.bfloat16),
            jax.ShapeDtypeStruct((heads, tok), jnp.float32),
        ),
        in_specs=[VMEM] * span_len,
        out_specs=(VMEM, VMEM),
        compiler_params=params(4),
        name="combine",
    )(*returned)
    other = lax.ppermute(attended, "head", [(0, 1), (1, 0)])
    shape = jax.ShapeDtypeStruct((tok, width), jnp.bfloat16)
    home = pl.pallas_call(
        project_home_kernel,
        out_shape=shape,
        in_specs=[VMEM, VMEM],
        out_specs=VMEM,
        cost_estimate=cost(2 * tok * heads * DH * width, heads * DH * width * 2),
        compiler_params=params(4),
        name="project_home",
    )(attended, weight)
    return pl.pallas_call(
        finish_kernel,
        out_shape=(shape, jax.ShapeDtypeStruct((heads, tok), jnp.float32)),
        in_specs=[VMEM, VMEM, VMEM, VMEM],
        out_specs=(HBM, HBM),
        scratch_shapes=[
            pltpu.VMEM((tok, width), jnp.bfloat16),
            pltpu.SemaphoreType.DMA((1 + width // math.gcd(width, OUT_STEP),)),
        ],
        compiler_params=params(4),
        name="finish",
    )(home, other, weight_away, log_sum)


def solution(mesh):
    in_specs = (
        P(("blk", "rep"), "head"),
        P(("blk", "rep"), "head"),
        P(("blk", "rep"), "head"),
        P(),
        P("head", None),
    )
    out_specs = (P(("blk", "rep"), "head"), P("head", ("blk", "rep")))

    return jax.shard_map(body, mesh=mesh, in_specs=in_specs, out_specs=out_specs, check_vma=False)
```

```python
import math

import jax
import jax.numpy as jnp
from jax import lax
from jax.experimental import pallas as pl
from jax.experimental.pallas import tpu as pltpu
from jax.sharding import PartitionSpec as P


GROUP = 3
DH = 128
NEG_FILL = -1e30
LOG2E = math.log2(math.e)
STAT_ROWS = 16


VMEM = pl.BlockSpec(memory_space=pltpu.VMEM)
HBM = pl.BlockSpec(memory_space=pltpu.HBM)


def source_of(me, hop, count):
    if count & (count - 1) == 0:
        return lax.bitwise_xor(me, jnp.int32(hop))
    return lax.rem(me + (count - hop), count)


def hops_out(hop, count):
    if count & (count - 1) == 0:
        return [(i, i ^ hop) for i in range(count)]
    return [(i, (i + hop) % count) for i in range(count)]


def hops_back(hop, count):
    return [(b, a) for a, b in hops_out(hop, count)]


def pack_kernel(
    spans, span_len, query_hbm, keys_hbm, values_hbm, order_hbm,
    query_ref, packed_ref, bound_ref, order_ref, sems,
):
    kv_heads, _, tok, _ = packed_ref.shape
    heads = query_ref.shape[0] // tok
    order_copy = pltpu.make_async_copy(order_hbm, order_ref, sems.at[0])
    copies = []
    for head in range(kv_heads):
        columns = pl.ds(head * DH, DH)
        copies.append((keys_hbm.at[:, columns], packed_ref.at[head, 0]))
        copies.append((values_hbm.at[:, columns], packed_ref.at[head, 1]))
    for head in range(heads):
        copies.append(
            (query_hbm.at[:, pl.ds(head * DH, DH)], query_ref.at[pl.ds(head * tok, tok), :])
        )
    copies = [
        pltpu.make_async_copy(source, target, sems.at[1 + at])
        for at, (source, target) in enumerate(copies)
    ]
    order_copy.start()
    for copy in copies:
        copy.start()
    order_copy.wait()
    blk_rank, rep_rank = lax.axis_index("blk"), lax.axis_index("rep")
    places = [
        blk_rank * span_len + source_of(rep_rank, hop, span_len) for hop in range(span_len)
    ]
    places += [source_of(blk_rank, hop, spans) * span_len + rep_rank for hop in range(spans)]
    for row, place in enumerate(places):
        bound_ref[row : row + 1, :] = jnp.full((1, tok), order_ref[place], jnp.int32)
    for copy in copies:
        copy.wait()


def prepare_kernel(*refs):
    kv_refs, (keys_ref, values_ref) = refs[:-2], refs[-2:]
    for at, ref in enumerate(kv_refs):
        kv_heads, _, tok, _ = ref.shape
        here = slice(at * tok, (at + 1) * tok)
        for kv_head in range(kv_heads):
            keys_ref[kv_head, here, :] = ref[kv_head, 0]
            values_ref[kv_head, :, here] = ref[kv_head, 1].T


def store_part(out_ref, kv_head, numer, top, total, factor):
    tok = out_ref.shape[1]
    heads = (out_ref.shape[0] - STAT_ROWS) // DH
    some = total > 0.0
    numer = (numer * jnp.where(some, 1.0 / total, 0.0)).astype(jnp.bfloat16)
    log_sum = top * factor + jnp.where(some, jnp.log(total), 0.0)
    high = log_sum.astype(jnp.bfloat16)
    rest = log_sum - high.astype(jnp.float32)
    middle = rest.astype(jnp.bfloat16)
    low = (rest - middle.astype(jnp.float32)).astype(jnp.bfloat16)
    for group in range(GROUP):
        head = kv_head * GROUP + group
        lanes = slice(group * tok, (group + 1) * tok)
        out_ref[head * DH : (head + 1) * DH, :] = numer[:, lanes]
        for at, stat in enumerate((high, middle, low)):
            row = heads * DH + 3 * head + at
            out_ref[row : row + 1, :] = stat[:, lanes]


def attend_kernel(rep_hop, spans, bound_ref, query_ref, keys_ref, values_ref, out_ref):
    tok = bound_ref.shape[1]
    kv_heads = keys_ref.shape[0]
    factor = DH**-0.5
    lanes = GROUP * tok
    for kv_head in range(kv_heads):
        query = query_ref[kv_head * lanes : (kv_head + 1) * lanes, :]
        scores, allowed, top = [], [], None
        for first in range(0, spans, 2):
            count = min(2, spans - first)
            raw = lax.dot_general(
                keys_ref[kv_head, first * tok : (first + count) * tok, :],
                query,
                (((1,), (1,)), ((), ())),
                preferred_element_type=jnp.float32,
            )
            for at in range(count):
                hop = first + at
                chunk = raw[at * tok : (at + 1) * tok, :]
                if rep_hop == 0 and hop == 0:
                    ahead = lax.broadcasted_iota(jnp.int32, (tok, tok), 0)
                    ahead = ahead - lax.broadcasted_iota(jnp.int32, (tok, tok), 1)
                    ahead = jnp.concatenate([ahead] * GROUP, axis=1)
                    chunk = jnp.where(ahead <= 0, chunk, NEG_FILL)
                row = bound_ref.shape[0] - spans + hop
                visible = bound_ref[rep_hop : rep_hop + 1, :] >= bound_ref[row : row + 1, :]
                scores.append(chunk)
                allowed.append(jnp.concatenate([visible.astype(jnp.int32)] * GROUP, axis=1) > 0)
                chunk_top = jnp.max(chunk, axis=0, keepdims=True)
                chunk_top = jnp.where(allowed[hop], chunk_top, NEG_FILL)
                top = chunk_top if top is None else jnp.maximum(top, chunk_top)
        total, numer = None, None
        for first in range(0, spans, 2):
            count, weights = min(2, spans - first), []
            for hop in range(first, first + count):
                chunk_top = jnp.where(allowed[hop], top, -NEG_FILL)
                weight = jnp.exp2((scores[hop] - chunk_top) * (factor * LOG2E))
                total = weight if total is None else total + weight
                weights.append(weight.astype(jnp.bfloat16))
            term = lax.dot_general(
                values_ref[kv_head, :, first * tok : (first + count) * tok],
                jnp.concatenate(weights, axis=0),
                (((1,), (0,)), ((), ())),
                preferred_element_type=jnp.float32,
            )
            numer = term if numer is None else numer + term
        total = jnp.sum(total, axis=0, keepdims=True)
        store_part(out_ref, kv_head, numer, top, total, factor)


def attend_fetch_kernel(spans, chunks, *refs):
    weight_hbm, part_ref, weight_ref, sems = refs[-4:]
    rows, width = weight_ref.shape[0] // chunks, weight_ref.shape[1]
    columns = pl.ds(pl.multiple_of(lax.axis_index("head") * width, 128), width)
    copies = []
    for chunk in range(chunks):
        here = pl.ds(chunk * rows, rows)
        copies.append(
            pltpu.make_async_copy(
                weight_hbm.at[here, columns], weight_ref.at[here, :], sems.at[chunk]
            )
        )
        copies[-1].start()
    attend_kernel(0, spans, *refs[:-4], part_ref)
    for copy in copies:
        copy.wait()


def gather_parts(part_refs, head, heads, merged=None):
    tops, totals, numers = [], [], []
    rows = slice(head * DH, (head + 1) * DH)
    if merged is not None:
        numer_ref, stat_ref = merged
        tops.append(stat_ref[head : head + 1, :])
        totals.append(stat_ref[heads + head : heads + head + 1, :])
        numers.append(numer_ref[rows, :])
    for part in part_refs:
        parts = part[heads * DH : heads * DH + STAT_ROWS, :].astype(jnp.float32)
        row = 3 * head
        tops.append(parts[row : row + 1] + parts[row + 1 : row + 2] + parts[row + 2 : row + 3])
        totals.append(None)
        numers.append(part[rows, :].astype(jnp.float32))
    top = tops[0]
    for other in tops[1:]:
        top = jnp.maximum(top, other)
    shares = [jnp.exp(other - top) for other in tops]
    total = None
    for share, amount in zip(shares, totals):
        term = share if amount is None else share * amount
        total = term if total is None else total + term
    return top, total, shares, numers


def merge_kernel(*refs):
    part_refs, (numer_ref, stat_ref) = refs[:-2], refs[-2:]
    heads = numer_ref.shape[0] // DH
    for head in range(heads):
        top, total, shares, numers = gather_parts(part_refs, head, heads)
        numer = None
        for share, values in zip(shares, numers):
            numer = values * share if numer is None else numer + values * share
        numer_ref[head * DH : (head + 1) * DH, :] = numer
        stat_ref[head : head + 1, :] = top
        stat_ref[heads + head : heads + head + 1, :] = total


def combine_kernel(numer_ref, stat_ref, *refs):
    part_refs, (attended_ref, log_sum_ref) = refs[:-2], refs[-2:]
    heads = log_sum_ref.shape[0]
    for head in range(heads):
        top, total, shares, numers = gather_parts(part_refs, head, heads, (numer_ref, stat_ref))
        scale = 1.0 / total
        numer = None
        for share, values in zip(shares, numers):
            term = values * (share * scale)
            numer = term if numer is None else numer + term
        attended_ref[head * DH : (head + 1) * DH, :] = numer.astype(jnp.bfloat16)
        log_sum_ref[head : head + 1, :] = top + jnp.log(total)


def project(attended_ref, weight_ref, columns):
    return lax.dot_general(
        attended_ref[...],
        weight_ref[:, columns],
        (((0,), (0,)), ((), ())),
        preferred_element_type=jnp.float32,
    ).astype(jnp.bfloat16)


def project_home_kernel(attended_ref, weight_ref, out_ref):
    out_ref[...] = project(attended_ref, weight_ref, slice(None))


def out_steps(width):
    unit = width // 6
    if unit % 128:
        return [width]
    return [4 * unit, 2 * unit]


def finish_kernel(
    home_ref, other_ref, weight_ref, log_ref, out_hbm, log_hbm, out_ref, sems
):
    width = out_ref.shape[1]
    log_copy = pltpu.make_async_copy(log_ref, log_hbm, sems.at[0])
    log_copy.start()
    base = lax.axis_index("head") * width
    copies, start = [log_copy], 0
    for at, step in enumerate(out_steps(width)):
        here = slice(start, start + step)
        columns = pl.ds(pl.multiple_of(base + start, 128), step)
        other = project(other_ref, weight_ref, columns)
        out_ref[:, here] = (
            home_ref[:, here].astype(jnp.float32) + other.astype(jnp.float32)
        ).astype(jnp.bfloat16)
        copies.append(
            pltpu.make_async_copy(out_ref.at[:, here], out_hbm.at[:, here], sems.at[1 + at])
        )
        copies[-1].start()
        start += step
    for copy in copies:
        copy.wait()


def cost(flops, moved, transcendentals=0):
    return pl.CostEstimate(flops=flops, bytes_accessed=moved, transcendentals=transcendentals)


def in_hbm(array):
    return pltpu.with_memory_space_constraint(array, pltpu.HBM)


def params(mib):
    return pltpu.CompilerParams(vmem_limit_bytes=mib * 2**20)


def body(queries, keys, values, stretch_order, out_weight):
    tok = queries.shape[0]
    kv_heads = keys.shape[1] // DH
    heads = kv_heads * GROUP
    width = out_weight.shape[1] // lax.axis_size("head")
    spans, span_len = lax.axis_size("blk"), lax.axis_size("rep")
    query, packed, bounds = pl.pallas_call(
        lambda *refs: pack_kernel(spans, span_len, *refs),
        out_shape=(
            jax.ShapeDtypeStruct((heads * tok, DH), jnp.bfloat16),
            jax.ShapeDtypeStruct((kv_heads, 2, tok, DH), jnp.bfloat16),
            jax.ShapeDtypeStruct((spans + span_len, tok), jnp.int32),
        ),
        in_specs=[HBM] * 4,
        out_specs=(VMEM, VMEM, VMEM),
        scratch_shapes=[
            pltpu.SMEM(stretch_order.shape, jnp.int32),
            pltpu.SemaphoreType.DMA((1 + 2 * kv_heads + heads,)),
        ],
        compiler_params=params(4),
        name="pack",
    )(*[in_hbm(x) for x in (queries, keys, values, stretch_order)])
    kv, query = [packed], [query]
    for hop in range(1, spans):
        kv.append(lax.ppermute(packed, "blk", hops_out(hop, spans)))
    for hop in range(1, span_len):
        query.append(lax.ppermute(query[0], "rep", hops_out(hop, span_len)))
    weight_away = lax.ppermute(out_weight, "head", [(0, 1), (1, 0)])
    keys_all, values_all = pl.pallas_call(
        prepare_kernel,
        out_shape=(
            jax.ShapeDtypeStruct((kv_heads, spans * tok, DH), jnp.bfloat16),
            jax.ShapeDtypeStruct((kv_heads, DH, spans * tok), jnp.bfloat16),
        ),
        in_specs=[VMEM] * spans,
        out_specs=(VMEM, VMEM),
        compiler_params=params(8),
        name="prepare",
    )(*kv)
    part_shape = jax.ShapeDtypeStruct((heads * DH + STAT_ROWS, tok), jnp.bfloat16)
    attend = dict(
        cost_estimate=cost(
            4 * heads * tok * spans * tok * DH,
            2 * heads * tok * DH * 2 + spans * tok * DH * 4,
            heads * tok * spans * tok,
        ),
        compiler_params=params(16 if spans > 8 else 8),
    )
    chunks = heads * DH // math.gcd(heads * DH, 64)
    parts = [None]
    for hop in range(1, span_len):
        parts.append(
            pl.pallas_call(
                lambda *refs, hop=hop: attend_kernel(hop, spans, *refs),
                out_shape=part_shape,
                in_specs=[VMEM] * 4,
                out_specs=VMEM,
                name="attend",
                **attend,
            )(bounds, query[hop], keys_all, values_all)
        )
    parts[0], weight = pl.pallas_call(
        lambda *refs: attend_fetch_kernel(spans, chunks, *refs),
        out_shape=(part_shape, jax.ShapeDtypeStruct((heads * DH, width), jnp.bfloat16)),
        in_specs=[VMEM] * 4 + [HBM],
        out_specs=(VMEM, VMEM),
        scratch_shapes=[pltpu.SemaphoreType.DMA((chunks,))],
        name="attend_fetch",
        **attend,
    )(bounds, query[0], keys_all, values_all, in_hbm(out_weight))
    returned = [parts[0]]
    for hop in range(1, span_len):
        returned.append(lax.ppermute(parts[hop], "rep", hops_back(hop, span_len)))
    early = min(2, span_len)
    merged = pl.pallas_call(
        merge_kernel,
        out_shape=(
            jax.ShapeDtypeStruct((heads * DH, tok), jnp.float32),
            jax.ShapeDtypeStruct((-(-2 * heads // 8) * 8, tok), jnp.float32),
        ),
        in_specs=[VMEM] * early,
        out_specs=(VMEM, VMEM),
        compiler_params=params(4),
        name="merge",
    )(*returned[:early])
    attended, log_sum = pl.pallas_call(
        combine_kernel,
        out_shape=(
            jax.ShapeDtypeStruct((heads * DH, tok), jnp.bfloat16),
            jax.ShapeDtypeStruct((heads, tok), jnp.float32),
        ),
        in_specs=[VMEM] * (2 + span_len - early),
        out_specs=(VMEM, VMEM),
        compiler_params=params(4),
        name="combine",
    )(*merged, *returned[early:])
    other = lax.ppermute(attended, "head", [(0, 1), (1, 0)])
    shape = jax.ShapeDtypeStruct((tok, width), jnp.bfloat16)
    home = pl.pallas_call(
        project_home_kernel,
        out_shape=shape,
        in_specs=[VMEM, VMEM],
        out_specs=VMEM,
        cost_estimate=cost(2 * tok * heads * DH * width, heads * DH * width * 2),
        compiler_params=params(4),
        name="project_home",
    )(attended, weight)
    return pl.pallas_call(
        finish_kernel,
        out_shape=(shape, jax.ShapeDtypeStruct((heads, tok), jnp.float32)),
        in_specs=[VMEM, VMEM, VMEM, VMEM],
        out_specs=(HBM, HBM),
        scratch_shapes=[
            pltpu.VMEM((tok, width), jnp.bfloat16),
            pltpu.SemaphoreType.DMA((1 + len(out_steps(width)),)),
        ],
        compiler_params=params(4),
        name="finish",
    )(home, other, weight_away, log_sum)


def solution(mesh):
    in_specs = (
        P(("blk", "rep"), "head"),
        P(("blk", "rep"), "head"),
        P(("blk", "rep"), "head"),
        P(),
        P("head", None),
    )
    out_specs = (P(("blk", "rep"), "head"), P("head", ("blk", "rep")))

    return jax.shard_map(body, mesh=mesh, in_specs=in_specs, out_specs=out_specs, check_vma=False)
```
